256 devices in a mesh: dp: 2 (over z_lo), expert: 128 (over y, z_hi, x, core).
Axes of the slice: x: 4, y: 4, z: 8 (z_hi: 4, z_lo: 2; z = z_hi * 2 + z_lo), core: 2. Of those that a mesh axis runs over, the one named last changes fastest.
Arguments:
- tokens: bfloat16 [32768, 2880], P('expert'), may hold values from -2 to 2
- segment_ids: int32 [32768], P('expert'), may hold values from 0 to 255, never falling along the last dimension, each value on 1 to 512 neighbouring positions
- expert_ids: int32 [32768, 4], P('expert'), may hold values from 0 to 127, as said below
- attn_gain: float32 [2880], replicated, may hold values from 0.1 to 1.9
- sinks: float32 [32], P('dp'), may hold values from 2 to 5
- qkv_master: float32 [2560, 2880], P(('dp', 'expert')), may hold values from -0.109375 to 0.109375
- qkv_mom: float32 [2560, 2880], P(('dp', 'expert')), may hold values from -0.006 to 0.006
- qkv_var: float32 [2560, 2880], P(('dp', 'expert')), may hold values from 1e-08 to 1e-06
- qkv_grad: float32 [2560, 2880], P(('dp', 'expert')), may hold values from -0.06 to 0.06
- o_master: float32 [2048, 2880], P(('dp', 'expert')), may hold values from -0.125 to 0.125
- o_mom: float32 [2048, 2880], P(('dp', 'expert')), may hold values from -0.006 to 0.006
- o_var: float32 [2048, 2880], P(('dp', 'expert')), may hold values from 1e-08 to 1e-06
- o_grad: float32 [2048, 2880], P(('dp', 'expert')), may hold values from -0.06 to 0.06
- router_weight: bfloat16 [2880, 128], replicated, may hold values from -0.109375 to 0.109375
- router_bias: float32 [128], replicated, may hold values from -4 to 4
- mlp_gain: float32 [2880], replicated, may hold values from 0.1 to 1.9
Outputs:
- dispatched: bfloat16 [128, 128, 2, 8, 2880], P('expert', None, 'dp')
- gate_slots: bfloat16 [128, 128, 2, 8], P('expert', None, 'dp')
The draws below stay inside these ranges and needn't reach their ends.
Inputs may be any that keep to these rules, and one draw needn't show every extreme that they name: `expert_ids`: each row names 4 different experts. In each aligned block of 128 rows no expert is named more than 8 times, and one expert, the same in every block of a draw, is named exactly 8 times in every block.
All inputs are finite; a program needn't handle non-finite values.
Results may differ from the reference program's by a relative error of at most 0.012.
The reference program's roundings to bfloat16 on the way count: a program that leaves them out, or rounds other values in their place, can miss the bound.
Values may be sent and summed in bfloat16 or wider, within the bound.
A program may use at most 128 MiB of HBM per device.

```python
import math
import jax
import jax.numpy as jnp
import numpy as np
from jax import lax

D = 2880
HEADS = 32
KV_HEADS = 4
HEAD_DIM = 64
WINDOW = 128
TOPK = 4
TOK_DEV = 256
EXPERTS = 128
TOKENS = 32768
BLOCK = 128
CAP = 8
QKV_ROWS = 2560
O_ROWS = 2048
N_DP = 2
N_EXPERT = 128


def draw_expert_ids(key, part):
    blocks = TOKENS // BLOCK
    pair_half = EXPERTS // 2
    base_key = jax.random.fold_in(key, 11)
    chosen = jax.random.randint(jax.random.fold_in(base_key, 1), (), 0, EXPERTS).astype(jnp.int32)

    def one_block(index):
        block_key = jax.random.fold_in(base_key, index + 7)
        ordering = jax.random.permutation(jax.random.fold_in(block_key, 1), EXPERTS).astype(jnp.int32)
        shares = jax.random.randint(jax.random.fold_in(block_key, 2), (pair_half,), 0, CAP + 1).astype(jnp.int32)
        where_pos = jnp.argmax(ordering == chosen).astype(jnp.int32)
        pair_pos = where_pos % pair_half
        forced = jnp.where(where_pos < pair_half, CAP, 0).astype(jnp.int32)
        shares = jnp.where(jnp.arange(pair_half, dtype=jnp.int32) == pair_pos, forced, shares)
        counts = jnp.zeros((EXPERTS,), jnp.int32).at[ordering].set(jnp.concatenate([shares, CAP - shares]))
        bounds = jnp.cumsum(counts)
        listing = jnp.searchsorted(bounds, jnp.arange(BLOCK * TOPK, dtype=jnp.int32), side='right').astype(jnp.int32)
        layout = listing.reshape(TOPK, BLOCK).T
        shuffle = jax.random.permutation(jax.random.fold_in(block_key, 3), BLOCK)
        return layout[shuffle]
    return jax.vmap(one_block)(jnp.arange(blocks, dtype=jnp.int32)).reshape(TOKENS, TOPK).astype(jnp.int32)


def block_levels(own_key, extent, cuts, least, top_value):
    factor_of = 1.0
    for dim, shards_of in cuts:
        heights = jax.random.uniform(jax.random.fold_in(jax.random.fold_in(own_key, 6), dim), (shards_of,), jnp.float32, least / len(cuts), top_value / len(cuts))
        factor_of = factor_of * jnp.repeat(jnp.exp(heights), extent[dim] // shards_of).reshape((-1,) + (1,) * (len(extent) - 1 - dim))
    return factor_of


def split_up(amount, total, reach, lean):
    weights = [(1 << 20) // math.isqrt(standing ** lean) + 1 for standing in range(2, amount + 1)]
    spare, given = total - reach - (amount - 1), [1] * (amount - 1)
    while spare > 0:
        candidates = [i for i in range(amount - 1) if given[i] < reach]
        mass, left = sum([weights[i] for i in candidates]), spare
        for i in candidates:
            extra = min(reach - given[i], max(1, left * weights[i] // mass), spare)
            given[i] = given[i] + extra
            spare = spare - extra
    return np.array([reach] + given)


def ragged_sizes(own_key, count, total, bound, skew):
    if count == 2:
        one = jax.random.randint(own_key, (), max(1, total - bound), min(bound, total - 1) + 1)
        return jnp.stack([one, total - one])
    tallies = jnp.asarray(split_up(count, total, bound, skew), jnp.int32)
    couples = (count - 1) // 2
    donor, sink = tallies[1:1 + 2 * couples:2], tallies[2:2 + 2 * couples:2]
    room = jnp.minimum(donor - 1, bound - sink)
    shifted = jax.random.randint(jax.random.fold_in(own_key, 1), (couples,), 0, 1 << 20) % (room + 1)
    tallies = tallies.at[1:1 + 2 * couples:2].set(donor - shifted).at[2:2 + 2 * couples:2].set(sink + shifted)
    return tallies[jax.random.permutation(jax.random.fold_in(own_key, 2), count)]


def noise(rng, dims, deviation, bound, split=(), kind=jnp.bfloat16):
    array = deviation * jax.random.normal(rng, dims, jnp.float32)
    if split:
        array = array * block_levels(rng, dims, split, -0.22, 0.18)
    return jnp.clip(array, -bound, bound).astype(kind)


def setup_inputs(seed: int = 0) -> dict:
    key_list = jax.random.split(jax.random.key(seed), 17)
    tokens = noise(key_list[0], (TOKENS, D), 0.3, 2.0, ((0, 128),))
    segment_ids = jnp.searchsorted(jnp.cumsum(ragged_sizes(key_list[1], TOKENS // 128, TOKENS, 512, 1)), jnp.arange(TOKENS), side="right").astype(jnp.int32)
    expert_ids = draw_expert_ids(jax.random.fold_in(key_list[16], 71), 0)
    attn_gain = jnp.clip(1.0 + 0.18 * jax.random.normal(key_list[3], (D,), jnp.float32), 0.1, 1.9)
    sinks = jnp.clip(2.0 + 3.0 * jax.random.uniform(key_list[4], (HEADS,), jnp.float32) ** block_levels(key_list[4], (HEADS,), ((0, 2),), -0.2, 0.2), 2.0, 5.0)
    qkv_master = noise(key_list[5], (QKV_ROWS, D), D ** -0.5, 0.109375, ((0, 256),), jnp.float32)
    qkv_mom = noise(key_list[6], (QKV_ROWS, D), 0.001, 0.006, ((0, 256),), jnp.float32)
    qkv_var = jnp.clip(jnp.exp(math.log(9.999999974752427e-07) - 4.6051702 * jax.random.uniform(key_list[7], (QKV_ROWS, D), jnp.float32) ** block_levels(key_list[7], (QKV_ROWS, D), ((0, 256),), -0.2, 0.2)), 9.99999993922529e-09, 9.999999974752427e-07)
    qkv_grad = noise(key_list[8], (QKV_ROWS, D), 0.01, 0.06, ((0, 256),), jnp.float32)
    o_master = noise(key_list[9], (O_ROWS, D), O_ROWS ** -0.5, 0.125, ((0, 256),), jnp.float32)
    o_mom = noise(key_list[10], (O_ROWS, D), 0.001, 0.006, ((0, 256),), jnp.float32)
    o_var = jnp.clip(jnp.exp(math.log(9.999999974752427e-07) - 4.6051702 * jax.random.uniform(key_list[11], (O_ROWS, D), jnp.float32) ** block_levels(key_list[11], (O_ROWS, D), ((0, 256),), -0.2, 0.2)), 9.99999993922529e-09, 9.999999974752427e-07)
    o_grad = noise(key_list[12], (O_ROWS, D), 0.01, 0.06, ((0, 256),), jnp.float32)
    router_weight = noise(key_list[13], (D, EXPERTS), D ** -0.5, 0.109375)
    router_bias = noise(key_list[14], (EXPERTS,), 1.0, 4.0, (), jnp.float32)
    mlp_gain = jnp.clip(1.0 + 0.18 * jax.random.normal(key_list[15], (D,), jnp.float32), 0.1, 1.9)
    return dict(tokens=tokens, segment_ids=segment_ids, expert_ids=expert_ids, attn_gain=attn_gain, sinks=sinks, qkv_master=qkv_master, qkv_mom=qkv_mom, qkv_var=qkv_var, qkv_grad=qkv_grad, o_master=o_master, o_mom=o_mom, o_var=o_var, o_grad=o_grad, router_weight=router_weight, router_bias=router_bias, mlp_gain=mlp_gain)


beta_one = 0.9
beta_two = 0.999
adam_step = 100
learn_rate = 0.02
adam_eps = 1e-08
norm_eps = 1e-05
rope_base = 150000.0
contract_rows = (((1,), (1,)), ((), ()))

def adam_weights(master, moment, second_mom, gradient):
    moment_new = beta_one * moment + (1.0 - beta_one) * gradient
    second_new = beta_two * second_mom + (1.0 - beta_two) * gradient * gradient
    fix_one = 1.0 - beta_one ** adam_step
    fix_two = 1.0 - beta_two ** adam_step
    update = moment_new / fix_one / (jnp.sqrt(second_new / fix_two) + adam_eps)
    return (master - learn_rate * update).astype(jnp.bfloat16)

def rms_scale(values, gain_vec):
    mean_sq = lax.optimization_barrier(jnp.mean(values * values, axis=-1, keepdims=True))
    return values * lax.rsqrt(mean_sq + norm_eps) * gain_vec

def rotate(values, positions):
    half_dim = values.shape[-1] // 2
    frequency = rope_base ** (-(jnp.arange(half_dim).astype(jnp.float32) * 2.0) / values.shape[-1])
    angles = positions[:, None] * frequency[None, :]
    cosine = jnp.cos(angles)[:, None, :]
    sine_vals = jnp.sin(angles)[:, None, :]
    first_half = values[..., :half_dim]
    second_half = values[..., half_dim:]
    return jnp.concatenate([first_half * cosine - second_half * sine_vals, second_half * cosine + first_half * sine_vals], axis=-1)

def attention(queries, key_rows, value_rows, segments, sink_logits):
    row_count = queries.shape[0]
    scale = queries.shape[-1] ** (-0.5)
    scores = jnp.einsum('tgrd,ugd->grtu', queries.astype(jnp.float32), key_rows.astype(jnp.float32)) * scale
    position = jnp.arange(row_count, dtype=jnp.int32)
    offset = position[:, None] - position[None, :]
    allowed = (segments[:, None] == segments[None, :]) & (offset >= 0) & (offset < WINDOW)
    weights = jnp.where(allowed, jnp.exp(scores), 0.0)
    sink_terms = jnp.exp(sink_logits).reshape(key_rows.shape[1], -1)[:, :, None]
    running = sink_terms + lax.optimization_barrier(jnp.sum(weights, axis=-1))
    attn_probs = (weights / running[..., None]).astype(jnp.bfloat16)
    attended = jnp.einsum('grtu,ugd->tgrd', attn_probs.astype(jnp.float32), value_rows.astype(jnp.float32))
    return attended.astype(jnp.bfloat16).reshape(row_count, -1)

def gate_values(logits, choices, experts):
    picked = choices[:, :, None] == jnp.arange(experts, dtype=jnp.int32)[None, None, :]
    chosen = lax.optimization_barrier(jnp.sum(jnp.where(picked, logits[:, None, :], 0.0), axis=-1))
    raised = jnp.exp(chosen)
    return raised / lax.optimization_barrier(jnp.sum(raised, axis=-1, keepdims=True))

def slot_targets(choices, capacity, experts):
    flat_ids = choices.reshape(-1).astype(jnp.int32)
    onehot = (flat_ids[:, None] == jnp.arange(experts, dtype=jnp.int32)[None, :]).astype(jnp.int32)
    earlier = jnp.cumsum(onehot, axis=0) - onehot
    slot_index = lax.optimization_barrier(jnp.sum(earlier * onehot, axis=1)).astype(jnp.int32)
    return flat_ids * capacity + slot_index

def reference(tokens, segment_ids, expert_ids, attn_gain, sinks, qkv_master, qkv_mom, qkv_var, qkv_grad, o_master, o_mom, o_var, o_grad, router_weight, router_bias, mlp_gain):
    qkv_weight = adam_weights(qkv_master, qkv_mom, qkv_var, qkv_grad)
    o_weight = adam_weights(o_master, o_mom, o_var, o_grad)
    group_rows = QKV_ROWS // N_DP
    q_rows = HEADS // N_DP * HEAD_DIM
    kv_rows = KV_HEADS // N_DP * HEAD_DIM
    repeat_count = HEADS // KV_HEADS
    positions = jnp.arange(TOK_DEV).astype(jnp.float32)

    def per_pack(pack_data):
        rows, segments, choices = pack_data
        normed = rms_scale(rows.astype(jnp.float32), attn_gain).astype(jnp.bfloat16)
        projected = lax.dot_general(normed, qkv_weight, contract_rows, preferred_element_type=jnp.float32)
        projected = projected.reshape(TOK_DEV, N_DP, group_rows)
        queries = rotate(projected[:, :, :q_rows].reshape(TOK_DEV, HEADS, HEAD_DIM), positions).astype(jnp.bfloat16)
        queries = queries.reshape(TOK_DEV, KV_HEADS, repeat_count, HEAD_DIM)
        key_rows = rotate(projected[:, :, q_rows:q_rows + kv_rows].reshape(TOK_DEV, KV_HEADS, HEAD_DIM), positions).astype(jnp.bfloat16)
        value_rows = projected[:, :, q_rows + kv_rows:].reshape(TOK_DEV, KV_HEADS, HEAD_DIM).astype(jnp.bfloat16)
        attended = attention(queries, key_rows, value_rows, segments, sinks)
        residual = rows.astype(jnp.float32) + jnp.dot(attended, o_weight, preferred_element_type=jnp.float32)
        moe_all = rms_scale(residual, mlp_gain).astype(jnp.bfloat16)
        payloads = []
        gate_lists = []
        for group_num in range(N_DP):
            row_start = group_num * BLOCK
            moe_in = moe_all[row_start:row_start + BLOCK]
            block_ids = choices[row_start:row_start + BLOCK]
            logits = jnp.dot(moe_in, router_weight, preferred_element_type=jnp.float32) + router_bias
            gate_vals = gate_values(logits, block_ids, EXPERTS)
            target = slot_targets(block_ids, CAP, EXPERTS)
            source_row = jnp.arange(BLOCK * TOPK, dtype=jnp.int32) // TOPK
            payload = jnp.zeros((EXPERTS * CAP, D), jnp.bfloat16).at[target].set(moe_in[source_row])
            slot_gates = jnp.zeros((EXPERTS * CAP,), jnp.bfloat16).at[target].set(gate_vals.reshape(-1).astype(jnp.bfloat16))
            payloads.append(payload.reshape(EXPERTS, CAP, D))
            gate_lists.append(slot_gates.reshape(EXPERTS, CAP))
        return (jnp.stack(payloads), jnp.stack(gate_lists))
    packed = (tokens.reshape(N_EXPERT, TOK_DEV, D), segment_ids.reshape(N_EXPERT, TOK_DEV), expert_ids.reshape(N_EXPERT, TOK_DEV, TOPK))
    payload_all, gates_all = lax.map(per_pack, packed)
    dispatched = jnp.transpose(payload_all, (2, 0, 1, 3, 4))
    gate_slots = jnp.transpose(gates_all, (2, 0, 1, 3))
    return (dispatched, gate_slots)
```

```python
import jax
import jax.numpy as jnp
import numpy as np
from jax import lax
from jax.experimental import pallas as pl
from jax.experimental.pallas import tpu as pltpu
from jax.sharding import PartitionSpec as P

HEADS = 32
KV_HEADS = 4
HEAD_DIM = 64
WINDOW = 128
WIDTH = 2880
WIDE = 2944
HALF = 1408
META = 2816
MESH = pl.DeviceIdType.MESH

beta_one = 0.9
beta_two = 0.999
adam_step = 100
learn_rate = 0.02
adam_eps = 1e-08
norm_eps = 1e-05
rope_base = 150000.0
contract_rows = (((1,), (1,)), ((), ()))


def adam_weights(master, moment, second_mom, gradient):
    moment_new = beta_one * moment + (1.0 - beta_one) * gradient
    second_new = beta_two * second_mom + (1.0 - beta_two) * gradient * gradient
    fix_one = 1.0 - beta_one**adam_step
    fix_two = 1.0 - beta_two**adam_step
    update = moment_new / fix_one / (jnp.sqrt(second_new / fix_two) + adam_eps)
    return (master - learn_rate * update).astype(jnp.bfloat16)


def rms_scale(values, gain_vec):
    mean_sq = jnp.mean(values * values, axis=-1, keepdims=True)
    return values * lax.rsqrt(mean_sq + norm_eps) * gain_vec


def rotate(values, positions):
    half_dim = values.shape[-1] // 2
    frequency = rope_base ** (-(jnp.arange(half_dim).astype(jnp.float32) * 2.0) / values.shape[-1])
    angles = positions[:, None] * frequency[None, :]
    cosine = jnp.cos(angles)[:, None, :]
    sine_vals = jnp.sin(angles)[:, None, :]
    first_half = values[..., :half_dim]
    second_half = values[..., half_dim:]
    return jnp.concatenate(
        [
            first_half * cosine - second_half * sine_vals,
            second_half * cosine + first_half * sine_vals,
        ],
        axis=-1,
    )


def attention(queries, key_rows, value_rows, segments, sink_logits):
    row_count = queries.shape[0]
    scale = queries.shape[-1] ** (-0.5)
    scores = (
        jnp.einsum("tgrd,ugd->grtu", queries, key_rows, preferred_element_type=jnp.float32) * scale
    )
    position = jnp.arange(row_count, dtype=jnp.int32)
    offset = position[:, None] - position[None, :]
    allowed = (segments[:, None] == segments[None, :]) & (offset >= 0) & (offset < WINDOW)
    weights = jnp.where(allowed, jnp.exp(scores), 0.0)
    sink_terms = jnp.exp(sink_logits).reshape(key_rows.shape[1], -1)[:, :, None]
    running = sink_terms + jnp.sum(weights, axis=-1)
    attn_probs = (weights / running[..., None]).astype(jnp.bfloat16)
    attended = jnp.einsum(
        "grtu,ugd->tgrd", attn_probs, value_rows, preferred_element_type=jnp.float32
    )
    return attended.astype(jnp.bfloat16).reshape(row_count, -1)


def gate_values(logits, choices, experts):
    picked = choices[:, :, None] == jnp.arange(experts, dtype=jnp.int32)[None, None, :]
    chosen = jnp.sum(jnp.where(picked, logits[:, None, :], 0.0), axis=-1)
    raised = jnp.exp(chosen)
    return raised / jnp.sum(raised, axis=-1, keepdims=True)


def slot_numbers(choices, experts):
    flat_ids = choices.reshape(-1)
    onehot = (flat_ids[:, None] == jnp.arange(experts, dtype=jnp.int32)[None, :]).astype(jnp.int32)
    earlier = jnp.cumsum(onehot, axis=0) - onehot
    return jnp.sum(earlier * onehot, axis=1).reshape(choices.shape)


def place():
    e = lax.axis_index("expert")
    core = lax.rem(e, 2)
    x = lax.rem(lax.div(e, 2), 4)
    z = lax.rem(lax.div(e, 8), 4)
    y = lax.div(e, 32)
    return e, y, z, x, core


def expert_at(y, z, x, core):
    return y * 32 + z * 8 + x * 2 + core


def step(position, by):
    return lax.rem(position + by, 4)


def greet(peers):
    barrier = pltpu.get_barrier_semaphore()
    for peer in peers:
        pl.semaphore_signal(barrier, inc=1, device_id={"expert": peer}, device_id_type=MESH)
    pl.semaphore_wait(barrier, len(peers))


def remote(src, dst, send_sem, recv_sem, peer):
    return pltpu.make_async_remote_copy(
        src_ref=src,
        dst_ref=dst,
        send_sem=send_sem,
        recv_sem=recv_sem,
        device_id={"expert": peer},
        device_id_type=MESH,
    )


def gather_kernel(a, b, o, ga, gb, go, send, recv, pair_send, pair_recv, local):
    _, y, z, x, core = place()
    middle = y * (1 - core) + x * core
    last = x * (1 - core) + y * core

    def peer(last_at, middle_at, z_at):
        return expert_at(
            middle_at * (1 - core) + last_at * core,
            z_at,
            last_at * (1 - core) + middle_at * core,
            core,
        )

    partner = expert_at(y, z, x, 1 - core)
    ring = [
        (peer(last, middle, step(z, 1)), peer(last, middle, step(z, 3))),
        (peer(last, step(middle, 1), z), peer(last, step(middle, 3), z)),
        (peer(step(last, 1), middle, z), peer(step(last, 3), middle, z)),
    ]
    greet([p for pair in ring for p in pair] + [partner])
    streams = ((a, ga), (b, gb), (o, go))
    up, down, far, far_two = 0, 1, 2, 3
    sent, copies = [], {}

    def go_on(s, stage, kind, src, dst, direction):
        copy = remote(
            src, dst, send.at[s, stage, kind], recv.at[s, stage, kind], ring[stage][direction]
        )
        copy.start()
        copies[s, stage, kind] = copy
        sent.append(copy)

    def to_partner(s, k, block):
        copy = remote(block, block, pair_send.at[s, k], pair_recv.at[s, k], partner)
        copy.start()
        copies[s, "pair", k] = copy
        sent.append(copy)

    own = []
    for s, (shard, full) in enumerate(streams):
        mine = full.at[core, last, middle, z]
        go_on(s, 0, up, shard, mine, 0)
        go_on(s, 0, down, shard, mine, 1)
        copy = pltpu.make_async_copy(shard, mine, local.at[s])
        copy.start()
        own.append(copy)
    for s, (_, full) in enumerate(streams):
        if s < 2:
            copies[s, 0, up].wait_recv()
            block = full.at[core, last, middle, step(z, 3)]
            go_on(s, 0, far, block, block, 0)
        else:
            copies[s, 0, down].wait_recv()
            block = full.at[core, last, middle, step(z, 1)]
            go_on(s, 0, far, block, block, 1)
    for s, (_, full) in enumerate(streams):
        copies[s, 0, down if s < 2 else up].wait_recv()
        copies[s, 0, far].wait_recv()
        own[s].wait()
        block = full.at[core, last, middle]
        go_on(s, 1, up, block, block, 0)
        go_on(s, 1, down, block, block, 1)
    for s, (_, full) in enumerate(streams):
        copies[s, 1, up].wait_recv()
        block = full.at[core, last, step(middle, 3), pl.ds(0, 2)]
        go_on(s, 1, far, block, block, 0)
        copies[s, 1, down].wait_recv()
        block = full.at[core, last, step(middle, 1), pl.ds(2, 2)]
        go_on(s, 1, far_two, block, block, 1)
    for s, (_, full) in enumerate(streams):
        copies[s, 1, far].wait_recv()
        copies[s, 1, far_two].wait_recv()
        block = full.at[core, last]
        go_on(s, 2, up, block, block, 0)
        go_on(s, 2, down, block, block, 1)
        to_partner(s, 0, block)
    for s, (_, full) in enumerate(streams):
        copies[s, 2, up].wait_recv()
        block = full.at[core, step(last, 3), pl.ds(0, 2)]
        go_on(s, 2, far, block, block, 0)
        to_partner(s, 1, full.at[core, step(last, 3)])
        copies[s, 2, down].wait_recv()
        block = full.at[core, step(last, 1), pl.ds(2, 2)]
        go_on(s, 2, far_two, block, block, 1)
        to_partner(s, 2, full.at[core, step(last, 1)])
    for s, (_, full) in enumerate(streams):
        copies[s, 2, far].wait_recv()
        to_partner(s, 3, full.at[core, step(last, 2), pl.ds(0, 2)])
        copies[s, 2, far_two].wait_recv()
        to_partner(s, 4, full.at[core, step(last, 2), pl.ds(2, 2)])
    for s in range(3):
        for k in range(5):
            copies[s, "pair", k].wait_recv()
    for copy in sent:
        copy.wait_send()


def gather_weights(a, b, o):
    return pl.pallas_call(
        gather_kernel,
        out_shape=[
            jax.ShapeDtypeStruct((2, 4, 4, 4) + v.shape, jnp.bfloat16) for v in (a, b, o)
        ],
        in_specs=[pl.BlockSpec(memory_space=pltpu.VMEM)] * 3,
        out_specs=[pl.BlockSpec(memory_space=pl.ANY)] * 3,
        scratch_shapes=[
            pltpu.SemaphoreType.DMA((3, 3, 4)),
            pltpu.SemaphoreType.DMA((3, 3, 4)),
            pltpu.SemaphoreType.DMA((3, 5)),
            pltpu.SemaphoreType.DMA((3, 5)),
            pltpu.SemaphoreType.DMA((3,)),
        ],
        compiler_params=pltpu.CompilerParams(collective_id=0, has_side_effects=True),
        name="gather_weights",
    )(a, b, o)


def gathered_experts():
    core, last, middle, z = np.meshgrid(
        np.arange(2), np.arange(4), np.arange(4), np.arange(4), indexing="ij"
    )
    y = np.where(core == 0, middle, last)
    x = np.where(core == 0, last, middle)
    return (((y * 4 + z) * 4 + x) * 2 + core).reshape(-1)


def dispatch_kernel(
    rows, got, ring_rows, payload, picks, zsend, zrecv, send_sem, recv_sem
):
    _, y, z, x, core = place()
    here = y * 8 + x * 2 + core
    above, below = expert_at(y, step(z, 1), x, core), expert_at(y, step(z, 3), x, core)

    def plane_expert(index):
        return lax.div(index, 8) * 32 + z * 8 + lax.rem(index, 8)

    barrier = pltpu.get_barrier_semaphore()
    for peer in (above, below):
        pl.semaphore_signal(barrier, inc=1, device_id={"expert": peer}, device_id_type=MESH)

    def signal_one(i, carry):
        peer = plane_expert(lax.rem(here + i, 32))
        pl.semaphore_signal(barrier, inc=1, device_id={"expert": peer}, device_id_type=MESH)
        return carry

    lax.fori_loop(1, 32, signal_one, 0)
    pl.semaphore_wait(barrier, 33)

    meta, first, second = pl.ds(META, 128), pl.ds(0, HALF), pl.ds(HALF, META - HALF)
    tail = pl.ds(HALF, WIDE - HALF)
    sent = []

    def pass_on(k, src, slot, lanes, peer):
        copy = remote(
            src.at[:, lanes], ring_rows.at[slot, :, lanes], zsend.at[k], zrecv.at[k], peer
        )
        copy.start()
        sent.append(copy)
        return copy

    low_meta = pass_on(0, rows, 0, meta, above)
    high_meta = pass_on(1, rows, 1, meta, below)
    low_first = pass_on(2, rows, 0, first, above)
    high_second = pass_on(3, rows, 1, second, below)
    low_second = pass_on(4, rows, 0, second, above)
    high_first = pass_on(5, rows, 1, first, below)

    def choose(block, source):
        data = source[:, META:WIDE].astype(jnp.float32)
        code = lax.broadcasted_iota(jnp.int32, (128, 256), 1).astype(jnp.float32)
        plane = z.astype(jnp.float32)
        hit = jnp.zeros((128, 256), jnp.float32)
        for k in range(4):
            same = (data[:, 72 + k : 73 + k] == code) & (data[:, 76 + k : 77 + k] == plane)
            hit = hit + jnp.where(same, 1.0, 0.0)
        picks[block] = hit.T.astype(jnp.bfloat16)

    def expand(block, source, start, tiles):
        def one(i, carry):
            lanes = pl.ds(pl.multiple_of(start + i * 128, 128), 128)
            slots = jnp.dot(picks[block], source[:, lanes], preferred_element_type=jnp.float32)
            payload[block, :, :, lanes] = slots.reshape(32, 8, 128).astype(jnp.bfloat16)
            return carry

        lax.fori_loop(0, tiles, one, 0)

    def deliver(block, z_at, lanes):
        row = expert_at(y, z_at, x, core)
        pltpu.make_async_copy(
            payload.at[block, here, :, lanes], got.at[row, :, lanes], recv_sem
        ).start()

        def one(i, carry):
            index = lax.rem(here + i, 32)
            remote(
                payload.at[block, index, :, lanes],
                got.at[row, :, lanes],
                send_sem,
                recv_sem,
                plane_expert(index),
            ).start()
            return carry

        lax.fori_loop(1, 32, one, 0)

    choose(0, rows)
    expand(0, rows, 0, 11)
    deliver(0, z, first)
    expand(0, rows, HALF, 12)
    deliver(0, z, tail)
    from_low, from_high, from_far = ring_rows.at[0], ring_rows.at[1], ring_rows.at[2]
    low_meta.wait_recv()
    far_meta = pass_on(6, from_low, 2, meta, above)
    high_meta.wait_recv()
    choose(1, from_low)
    choose(2, from_high)
    low_first.wait_recv()
    far_first = pass_on(7, from_low, 2, first, above)
    high_second.wait_recv()
    far_second = pass_on(8, from_high, 2, second, below)
    expand(1, from_low, 0, 11)
    deliver(1, step(z, 3), first)
    expand(2, from_high, HALF, 12)
    deliver(2, step(z, 1), tail)
    far_meta.wait_recv()
    choose(3, from_far)
    low_second.wait_recv()
    expand(1, from_low, HALF, 12)
    deliver(1, step(z, 3), tail)
    high_first.wait_recv()
    expand(2, from_high, 0, 11)
    deliver(2, step(z, 1), first)
    far_first.wait_recv()
    expand(3, from_far, 0, 11)
    deliver(3, step(z, 2), first)
    far_second.wait_recv()
    expand(3, from_far, HALF, 12)
    deliver(3, step(z, 2), tail)
    pltpu.make_async_copy(got, got, recv_sem).wait()
    part = payload.at[:, pl.ds(0, 31)]
    pltpu.make_async_copy(part, part, send_sem).wait()
    for copy in sent:
        copy.wait_send()


def dispatch_rows(rows):
    return pl.pallas_call(
        dispatch_kernel,
        out_shape=jax.ShapeDtypeStruct((128, 8, WIDE), jnp.bfloat16),
        in_specs=[pl.BlockSpec(memory_space=pltpu.VMEM)],
        out_specs=pl.BlockSpec(memory_space=pl.ANY),
        scratch_shapes=[
            pltpu.VMEM((3, 128, WIDE), jnp.bfloat16),
            pltpu.VMEM((4, 32, 8, WIDE), jnp.bfloat16),
            pltpu.VMEM((4, 256, 128), jnp.bfloat16),
            pltpu.SemaphoreType.DMA((9,)),
            pltpu.SemaphoreType.DMA((9,)),
            pltpu.SemaphoreType.DMA,
            pltpu.SemaphoreType.DMA,
        ],
        compiler_params=pltpu.CompilerParams(collective_id=1, has_side_effects=True),
        name="dispatch_rows",
    )(rows)


def sent_and_summed(shard, axis, dim):
    devices = lax.axis_size(axis)
    before, after = (shard.shape[:dim], shard.shape[dim + 1 :])
    blocks = jnp.moveaxis(shard.reshape(*before, devices, -1, *after), dim, 0)
    tiles = lax.all_to_all(blocks, axis, 0, 0, tiled=True)
    return jnp.sum(tiles.astype(jnp.float32), axis=0)


def on_device(
    tokens,
    segment_ids,
    expert_ids,
    attn_gain,
    sinks,
    qkv_master,
    qkv_mom,
    qkv_var,
    qkv_grad,
    o_master,
    o_mom,
    o_var,
    o_grad,
    router_weight,
    router_bias,
    mlp_gain,
):
    tok_rows = tokens.shape[0]
    groups = lax.axis_size("dp")
    half_rows = tok_rows // groups
    group_index = lax.axis_index("dp")
    expert_index = lax.axis_index("expert")
    heads_here = sinks.shape[0]
    kv_here = KV_HEADS * heads_here // HEADS
    repeat_count = heads_here // kv_here
    q_rows = heads_here * HEAD_DIM
    kv_rows = kv_here * HEAD_DIM
    qkv_local = adam_weights(qkv_master, qkv_mom, qkv_var, qkv_grad)
    o_local = adam_weights(o_master, o_mom, o_var, o_grad)
    qkv_eight, qkv_two, o_full = gather_weights(qkv_local[:8], qkv_local[8:], o_local)
    order = gathered_experts()
    qkv_order = np.concatenate(
        [
            (order[:, None] * 10 + np.arange(8)[None, :]).reshape(-1),
            (order[:, None] * 10 + np.arange(8, 10)[None, :]).reshape(-1),
        ]
    ).astype(np.int32)
    o_order = (order[:, None] * 8 + np.arange(8)[None, :]).reshape(-1).astype(np.int32)
    normed = rms_scale(tokens.astype(jnp.float32), attn_gain).astype(jnp.bfloat16)
    qkv_eight = qkv_eight.reshape(-1, WIDTH)
    qkv_two = qkv_two.reshape(-1, WIDTH)
    shuffled = jnp.concatenate(
        [
            lax.dot_general(normed, w, contract_rows, preferred_element_type=jnp.float32)
            for w in (qkv_eight, qkv_two)
        ],
        axis=1,
    )
    high = lax.reduce_precision(shuffled, 8, 7)
    parts = jnp.concatenate([high, shuffled - high], axis=0).astype(jnp.bfloat16)
    width_here = q_rows + 2 * kv_rows
    unshuffle = (
        jnp.asarray(qkv_order)[:, None] == jnp.arange(width_here, dtype=jnp.int32)[None, :]
    ).astype(jnp.bfloat16)
    both = jnp.dot(parts, unshuffle, preferred_element_type=jnp.float32)
    projected = both[:tok_rows] + both[tok_rows:]
    positions = jnp.arange(tok_rows).astype(jnp.float32)
    queries = rotate(
        projected[:, :q_rows].reshape(tok_rows, heads_here, HEAD_DIM), positions
    ).astype(jnp.bfloat16)
    queries = queries.reshape(tok_rows, kv_here, repeat_count, HEAD_DIM)
    key_rows = rotate(
        projected[:, q_rows : q_rows + kv_rows].reshape(tok_rows, kv_here, HEAD_DIM), positions
    ).astype(jnp.bfloat16)
    value_rows = (
        projected[:, q_rows + kv_rows :].reshape(tok_rows, kv_here, HEAD_DIM).astype(jnp.bfloat16)
    )
    attended = attention(queries, key_rows, value_rows, segment_ids, sinks)
    shuffle = (
        jnp.arange(q_rows, dtype=jnp.int32)[:, None] == jnp.asarray(o_order)[None, :]
    ).astype(jnp.bfloat16)
    attended = jnp.dot(attended, shuffle, preferred_element_type=jnp.float32).astype(jnp.bfloat16)
    update = jnp.dot(attended, o_full.reshape(-1, WIDTH), preferred_element_type=jnp.float32)
    summed = sent_and_summed(update.astype(jnp.bfloat16), "dp", 0)
    own_rows = lax.dynamic_slice_in_dim(tokens, group_index * half_rows, half_rows, 0)
    own_choices = lax.dynamic_slice_in_dim(expert_ids, group_index * half_rows, half_rows, 0)
    residual = own_rows.astype(jnp.float32) + summed
    moe_in = rms_scale(residual, mlp_gain).astype(jnp.bfloat16)
    logits = jnp.dot(moe_in, router_weight, preferred_element_type=jnp.float32) + router_bias
    experts = router_weight.shape[1]
    gate_vals = gate_values(logits, own_choices, experts).astype(jnp.bfloat16)
    slots = slot_numbers(own_choices, experts)
    code = (own_choices // 32 * 8 + own_choices % 8) * 8 + slots
    plane = own_choices // 8 % 4
    extra = jnp.concatenate(
        [
            gate_vals,
            own_choices.astype(jnp.bfloat16),
            code.astype(jnp.bfloat16),
            plane.astype(jnp.bfloat16),
            jnp.zeros((half_rows, WIDE - WIDTH - 16), jnp.bfloat16),
        ],
        axis=1,
    )
    got = dispatch_rows(jnp.concatenate([moe_in, extra], axis=1))
    dispatched = got[:, :, :WIDTH][None, :, None]
    asked = got[:, :, WIDTH + 4 : WIDTH + 8].astype(jnp.float32) == expert_index.astype(jnp.float32)
    gates = jnp.sum(
        jnp.where(asked, got[:, :, WIDTH : WIDTH + 4].astype(jnp.float32), 0.0), axis=-1
    ).astype(jnp.bfloat16)
    return (dispatched, gates[None, :, None])


def solution(mesh):
    return jax.shard_map(
        on_device,
        mesh=mesh,
        in_specs=(
            P("expert", None),
            P("expert"),
            P("expert", None),
            P(),
            P("dp"),
            P(("dp", "expert"), None),
            P(("dp", "expert"), None),
            P(("dp", "expert"), None),
            P(("dp", "expert"), None),
            P(("dp", "expert"), None),
            P(("dp", "expert"), None),
            P(("dp", "expert"), None),
            P(("dp", "expert"), None),
            P(),
            P(),
            P(),
        ),
        out_specs=(P("expert", None, "dp", None, None), P("expert", None, "dp", None)),
        check_vma=False,
    )
```

```python
import jax
import jax.numpy as jnp
import numpy as np
from jax import lax
from jax.experimental import pallas as pl
from jax.experimental.pallas import tpu as pltpu
from jax.sharding import PartitionSpec as P

HEADS = 32
KV_HEADS = 4
HEAD_DIM = 64
WINDOW = 128
WIDTH = 2880
WIDE = 2944
HALF = 1408
META = 2816
MESH = pl.DeviceIdType.MESH
GATHER_SPACE = pl.ANY
FINISH_LANES = 768

beta_one = 0.9
beta_two = 0.999
adam_step = 100
learn_rate = 0.02
adam_eps = 1e-08
norm_eps = 1e-05
rope_base = 150000.0
contract_rows = (((1,), (1,)), ((), ()))


def adam_weights(master, moment, second_mom, gradient):
    moment_new = beta_one * moment + (1.0 - beta_one) * gradient
    second_new = beta_two * second_mom + (1.0 - beta_two) * gradient * gradient
    fix_one = 1.0 - beta_one**adam_step
    fix_two = 1.0 - beta_two**adam_step
    update = moment_new / fix_one / (jnp.sqrt(second_new / fix_two) + adam_eps)
    return (master - learn_rate * update).astype(jnp.bfloat16)


def rms_scale(values, gain_vec):
    mean_sq = jnp.mean(values * values, axis=-1, keepdims=True)
    return values * lax.rsqrt(mean_sq + norm_eps) * gain_vec


def rotate(values, positions):
    half_dim = values.shape[-1] // 2
    frequency = rope_base ** (-(jnp.arange(half_dim).astype(jnp.float32) * 2.0) / values.shape[-1])
    angles = positions[:, None] * frequency[None, :]
    cosine = jnp.cos(angles)[:, None, :]
    sine_vals = jnp.sin(angles)[:, None, :]
    first_half = values[..., :half_dim]
    second_half = values[..., half_dim:]
    return jnp.concatenate(
        [
            first_half * cosine - second_half * sine_vals,
            second_half * cosine + first_half * sine_vals,
        ],
        axis=-1,
    )


def attention(queries, key_rows, value_rows, segments, sink_logits):
    row_count = queries.shape[0]
    scale = queries.shape[-1] ** (-0.5)
    scores = (
        jnp.einsum("tgrd,ugd->grtu", queries, key_rows, preferred_element_type=jnp.float32) * scale
    )
    position = jnp.arange(row_count, dtype=jnp.int32)
    offset = position[:, None] - position[None, :]
    allowed = (segments[:, None] == segments[None, :]) & (offset >= 0) & (offset < WINDOW)
    weights = jnp.where(allowed, jnp.exp(scores), 0.0)
    sink_terms = jnp.exp(sink_logits).reshape(key_rows.shape[1], -1)[:, :, None]
    running = sink_terms + jnp.sum(weights, axis=-1)
    attn_probs = (weights / running[..., None]).astype(jnp.bfloat16)
    attended = jnp.einsum(
        "grtu,ugd->tgrd", attn_probs, value_rows, preferred_element_type=jnp.float32
    )
    return attended.astype(jnp.bfloat16).reshape(row_count, -1)


def gate_values(logits, choices, experts):
    picked = choices[:, :, None] == jnp.arange(experts, dtype=jnp.int32)[None, None, :]
    chosen = jnp.sum(jnp.where(picked, logits[:, None, :], 0.0), axis=-1)
    raised = jnp.exp(chosen)
    return raised / jnp.sum(raised, axis=-1, keepdims=True)


def slot_numbers(choices, experts):
    flat_ids = choices.reshape(-1)
    onehot = (flat_ids[:, None] == jnp.arange(experts, dtype=jnp.int32)[None, :]).astype(jnp.int32)
    earlier = jnp.cumsum(onehot, axis=0) - onehot
    return jnp.sum(earlier * onehot, axis=1).reshape(choices.shape)


def place():
    e = lax.axis_index("expert")
    core = lax.rem(e, 2)
    x = lax.rem(lax.div(e, 2), 4)
    z = lax.rem(lax.div(e, 8), 4)
    y = lax.div(e, 32)
    return e, y, z, x, core


def expert_at(y, z, x, core):
    return y * 32 + z * 8 + x * 2 + core


def step(position, by):
    return lax.rem(position + by, 4)


def greet(peers):
    barrier = pltpu.get_barrier_semaphore()
    for peer in peers:
        pl.semaphore_signal(barrier, inc=1, device_id={"expert": peer}, device_id_type=MESH)
    pl.semaphore_wait(barrier, len(peers))


def remote(src, dst, send_sem, recv_sem, peer):
    return pltpu.make_async_remote_copy(
        src_ref=src,
        dst_ref=dst,
        send_sem=send_sem,
        recv_sem=recv_sem,
        device_id={"expert": peer},
        device_id_type=MESH,
    )


def gather_kernel(a, b, o, ga, gb, go, send, recv, local):
    _, y, z, x, core = place()
    middle = y * (1 - core) + x * core
    last = x * (1 - core) + y * core

    def peer(last_at, middle_at, z_at):
        return expert_at(
            middle_at * (1 - core) + last_at * core,
            z_at,
            last_at * (1 - core) + middle_at * core,
            core,
        )

    partner = expert_at(y, z, x, 1 - core)
    ring = [
        (peer(last, middle, step(z, 1)), peer(last, middle, step(z, 3))),
        (peer(last, step(middle, 1), z), peer(last, step(middle, 3), z)),
        (peer(step(last, 1), middle, z), peer(step(last, 3), middle, z)),
    ]
    greet([p for pair in ring for p in pair] + [partner])
    streams = ((a, ga), (b, gb), (o, go))
    copies = {}

    def move(s, tag, src, dst, to):
        k = sum(1 for key in copies if key[0] == s)
        copy = remote(src, dst, send.at[s, k], recv.at[s, k], to)
        copy.start()
        copies[s, tag] = copy

    def arrived(s, tag):
        copies[s, tag].wait_recv()

    fine = ((0, 0, 4), (3, 0, 4), (1, 0, 4), (2, 0, 2), (2, 2, 2))
    coarse = (None,)
    pieces = (fine, coarse, fine)

    def part(s, last_by, k):
        full = streams[s][1]
        piece = pieces[s][k]
        if piece is None:
            return full.at[core, step(last, last_by)]
        return full.at[core, step(last, last_by), step(middle, piece[0]), pl.ds(piece[1], piece[2])]

    def along_last(s, k):
        block = part(s, 0, k)
        move(s, ("last", k, 0), block, block, ring[2][0])
        move(s, ("last", k, 1), block, block, ring[2][1])
        move(s, ("pair", 0, k), block, block, partner)

    def from_last(s, k):
        count = len(pieces[s])
        low, high = part(s, 3, k), part(s, 1, k)
        arrived(s, ("last", k, 0))
        if k < 2 and count > 1:
            move(s, ("far", k), low, low, ring[2][0])
        move(s, ("pair", 3, k), low, low, partner)
        arrived(s, ("last", k, 1))
        if k >= 2 or count == 1:
            move(s, ("far", k), high, high, ring[2][1])
        move(s, ("pair", 1, k), high, high, partner)

    own = []
    for s, (shard, full) in enumerate(streams):
        mine = full.at[core, last, middle, z]
        move(s, "z up", shard, mine, ring[0][0])
        move(s, "z down", shard, mine, ring[0][1])
        copy = pltpu.make_async_copy(shard, mine, local.at[s])
        copy.start()
        own.append(copy)
    for s, (_, full) in enumerate(streams):
        if s < 2:
            arrived(s, "z up")
            block = full.at[core, last, middle, step(z, 3)]
            move(s, "z far", block, block, ring[0][0])
        else:
            arrived(s, "z down")
            block = full.at[core, last, middle, step(z, 1)]
            move(s, "z far", block, block, ring[0][1])
    for s, (_, full) in enumerate(streams):
        arrived(s, "z down" if s < 2 else "z up")
        arrived(s, "z far")
        own[s].wait()
        block = full.at[core, last, middle]
        move(s, "middle up", block, block, ring[1][0])
        move(s, "middle down", block, block, ring[1][1])
        if s != 1:
            along_last(s, 0)
    for s, (_, full) in enumerate(streams):
        arrived(s, "middle up")
        block = full.at[core, last, step(middle, 3), pl.ds(0, 2)]
        move(s, "middle far 0", block, block, ring[1][0])
        if s != 1:
            along_last(s, 1)
        arrived(s, "middle down")
        block = full.at[core, last, step(middle, 1), pl.ds(2, 2)]
        move(s, "middle far 1", block, block, ring[1][1])
        if s != 1:
            along_last(s, 2)
    for s in range(3):
        arrived(s, "middle far 0")
        if s != 1:
            along_last(s, 3)
        arrived(s, "middle far 1")
        along_last(s, 4 if s != 1 else 0)
    for k in range(5):
        for s in range(3):
            if k < len(pieces[s]):
                from_last(s, k)
    for k in range(5):
        for s in range(3):
            if k < len(pieces[s]):
                block = part(s, 2, k)
                arrived(s, ("far", k))
                move(s, ("pair", 2, k), block, block, partner)
    for (s, tag), copy in copies.items():
        if tag[0] == "pair":
            copy.wait_recv()
    for copy in copies.values():
        copy.wait_send()


def gather_weights(a, b, o):
    return pl.pallas_call(
        gather_kernel,
        out_shape=[
            jax.ShapeDtypeStruct((2, 4, 4, 4) + v.shape, jnp.bfloat16) for v in (a, b, o)
        ],
        in_specs=[pl.BlockSpec(memory_space=pltpu.VMEM)] * 3,
        out_specs=[pl.BlockSpec(memory_space=GATHER_SPACE)] * 3,
        scratch_shapes=[
            pltpu.SemaphoreType.DMA((3, 42)),
            pltpu.SemaphoreType.DMA((3, 42)),
            pltpu.SemaphoreType.DMA((3,)),
        ],
        compiler_params=pltpu.CompilerParams(collective_id=0, has_side_effects=True),
        name="gather_weights",
    )(a, b, o)


def gathered_experts():
    core, last, middle, z = np.meshgrid(
        np.arange(2), np.arange(4), np.arange(4), np.arange(4), indexing="ij"
    )
    y = np.where(core == 0, middle, last)
    x = np.where(core == 0, last, middle)
    return (((y * 4 + z) * 4 + x) * 2 + core).reshape(-1)


def dispatch_kernel(
    rows, got, ring_rows, payload, picks, zsend, zrecv, send_sem, recv_sem
):
    _, y, z, x, core = place()
    here = y * 8 + x * 2 + core
    above, below = expert_at(y, step(z, 1), x, core), expert_at(y, step(z, 3), x, core)

    def plane_expert(index):
        return lax.div(index, 8) * 32 + z * 8 + lax.rem(index, 8)

    barrier = pltpu.get_barrier_semaphore()
    for peer in (above, below):
        pl.semaphore_signal(barrier, inc=1, device_id={"expert": peer}, device_id_type=MESH)

    def signal_one(i, carry):
        peer = plane_expert(lax.rem(here + i, 32))
        pl.semaphore_signal(barrier, inc=1, device_id={"expert": peer}, device_id_type=MESH)
        return carry

    lax.fori_loop(1, 32, signal_one, 0)
    pl.semaphore_wait(barrier, 33)

    meta = pl.ds(META, 128)
    chunks = ((0, 768), (768, 768), (1536, 768), (2304, 512))
    from_low, from_high, from_far = ring_rows.at[0], ring_rows.at[1], ring_rows.at[2]

    def pass_on(k, src, slot, lanes, peer):
        copy = remote(
            src.at[:, lanes], ring_rows.at[slot, :, lanes], zsend.at[k], zrecv.at[k], peer
        )
        copy.start()
        return copy

    def leg(n):
        if n < 4:
            up = pass_on(2 * n, rows, 0, pl.ds(*chunks[n]), above)
            down = pass_on(2 * n + 1, rows, 1, pl.ds(*chunks[3 - n]), below)
        else:
            up = pass_on(2 * n, from_low, 2, pl.ds(*chunks[n - 4]), above)
            down = pass_on(2 * n + 1, from_high, 2, pl.ds(*chunks[7 - n]), below)
        return up, down

    low_meta = pass_on(12, rows, 0, meta, above)
    high_meta = pass_on(13, rows, 1, meta, below)
    legs = [leg(0)]

    def choose(block, source):
        data = source[:, META:WIDE].astype(jnp.float32)
        code = lax.broadcasted_iota(jnp.int32, (128, 256), 1).astype(jnp.float32)
        plane = z.astype(jnp.float32)
        hit = jnp.zeros((128, 256), jnp.float32)
        for k in range(4):
            same = (data[:, 72 + k : 73 + k] == code) & (data[:, 76 + k : 77 + k] == plane)
            hit = hit + jnp.where(same, 1.0, 0.0)
        picks[block] = hit.T.astype(jnp.bfloat16)

    def deliver(block, source, z_at, chunk):
        start, lanes_here = chunks[chunk]
        lanes_here = lanes_here if chunk < 3 else WIDE - start
        for at in range(0, lanes_here, 384):
            lanes = pl.ds(start + at, min(384, lanes_here - at))
            slots = jnp.dot(picks[block], source[:, lanes], preferred_element_type=jnp.float32)
            payload[block, :, :, lanes] = slots.reshape(32, 8, -1).astype(jnp.bfloat16)
        lanes = pl.ds(start, lanes_here)
        row = expert_at(y, z_at, x, core)
        pltpu.make_async_copy(
            payload.at[block, here, :, lanes], got.at[row, :, lanes], recv_sem
        ).start()

        def one(i, carry):
            index = lax.rem(here + i, 32)
            remote(
                payload.at[block, index, :, lanes],
                got.at[row, :, lanes],
                send_sem,
                recv_sem,
                plane_expert(index),
            ).start()
            return carry

        lax.fori_loop(1, 32, one, 0)

    choose(0, rows)
    for chunk in range(4):
        deliver(0, rows, z, chunk)
    low_meta.wait_recv()
    far_meta = pass_on(14, from_low, 2, meta, above)
    high_meta.wait_recv()
    choose(1, from_low)
    choose(2, from_high)
    for n in range(6):
        up, down = legs[n]
        if n < 5:
            up.wait_send()
            down.wait_send()
            legs.append(leg(n + 1))
        if n == 3:
            far_meta.wait_recv()
            choose(3, from_far)
        up.wait_recv()
        deliver(*((1, from_low, step(z, 3), n) if n < 4 else (3, from_far, step(z, 2), n - 4)))
        down.wait_recv()
        deliver(*((2, from_high, step(z, 1), 3 - n) if n < 4 else (3, from_far, step(z, 2), 7 - n)))
    pltpu.make_async_copy(got, got, recv_sem).wait()
    part = payload.at[:, pl.ds(0, 31)]
    pltpu.make_async_copy(part, part, send_sem).wait()
    for copy in (low_meta, high_meta, far_meta) + legs[5]:
        copy.wait_send()


def dispatch_rows(rows):
    return pl.pallas_call(
        dispatch_kernel,
        out_shape=jax.ShapeDtypeStruct((128, 8, WIDE), jnp.bfloat16),
        in_specs=[pl.BlockSpec(memory_space=pltpu.VMEM)],
        out_specs=pl.BlockSpec(memory_space=pl.ANY),
        scratch_shapes=[
            pltpu.VMEM((3, 128, WIDE), jnp.bfloat16),
            pltpu.VMEM((4, 32, 8, WIDE), jnp.bfloat16),
            pltpu.VMEM((4, 256, 128), jnp.bfloat16),
            pltpu.SemaphoreType.DMA((15,)),
            pltpu.SemaphoreType.DMA((15,)),
            pltpu.SemaphoreType.DMA,
            pltpu.SemaphoreType.DMA,
        ],
        compiler_params=pltpu.CompilerParams(collective_id=1, has_side_effects=True),
        name="dispatch_rows",
    )(rows)


def finish_kernel(got, out, gates):
    spot = pl.program_id(0)
    lanes_here = got.shape[2]
    halves = []
    for part in range(2):
        rows = got[part * 64 : part * 64 + 64].reshape(512, lanes_here)
        source = lax.broadcasted_iota(jnp.int32, (512, 512), 0)
        target = lax.broadcasted_iota(jnp.int32, (512, 512), 1)
        pick = (source == (target & 63) * 8 + (target >> 6)).astype(jnp.bfloat16)
        halves.append(
            lax.dot_general(rows, pick, (((0,), (0,)), ((), ())), preferred_element_type=jnp.float32)
        )
    whole = []
    for c in range(8):
        cut = slice(c * 64, c * 64 + 64)
        whole.append(jnp.concatenate([halves[0][:, cut], halves[1][:, cut]], axis=1))
        out[c] = whole[c].astype(jnp.bfloat16)

    @pl.when(spot == WIDTH // FINISH_LANES)
    def _():
        mine = lax.axis_index("expert").astype(jnp.float32)
        first = WIDTH % FINISH_LANES
        for c in range(8):
            data = whole[c][first : first + 8]
            asked = jnp.where(data[4:8] == mine, data[:4], 0.0)
            gates[c : c + 1] = jnp.sum(asked, axis=0, keepdims=True)


def finish(got):
    return pl.pallas_call(
        finish_kernel,
        grid=(-(-WIDE // FINISH_LANES),),
        out_shape=[
            jax.ShapeDtypeStruct((8, WIDTH, 128), jnp.bfloat16),
            jax.ShapeDtypeStruct((8, 128), jnp.float32),
        ],
        in_specs=[pl.BlockSpec((128, 8, FINISH_LANES), lambda i: (0, 0, i))],
        out_specs=[
            pl.BlockSpec((8, FINISH_LANES, 128), lambda i: (0, i, 0)),
            pl.BlockSpec((8, 128), lambda i: (0, 0)),
        ],
        name="finish",
    )(got)


def sent_and_summed(shard, axis, dim):
    devices = lax.axis_size(axis)
    before, after = (shard.shape[:dim], shard.shape[dim + 1 :])
    blocks = jnp.moveaxis(shard.reshape(*before, devices, -1, *after), dim, 0)
    tiles = lax.all_to_all(blocks, axis, 0, 0, tiled=True)
    return jnp.sum(tiles.astype(jnp.float32), axis=0)


def on_device(
    tokens,
    segment_ids,
    expert_ids,
    attn_gain,
    sinks,
    qkv_master,
    qkv_mom,
    qkv_var,
    qkv_grad,
    o_master,
    o_mom,
    o_var,
    o_grad,
    router_weight,
    router_bias,
    mlp_gain,
):
    tok_rows = tokens.shape[0]
    groups = lax.axis_size("dp")
    half_rows = tok_rows // groups
    group_index = lax.axis_index("dp")
    heads_here = sinks.shape[0]
    kv_here = KV_HEADS * heads_here // HEADS
    repeat_count = heads_here // kv_here
    q_rows = heads_here * HEAD_DIM
    kv_rows = kv_here * HEAD_DIM
    qkv_local = adam_weights(qkv_master, qkv_mom, qkv_var, qkv_grad)
    o_local = adam_weights(o_master, o_mom, o_var, o_grad)
    qkv_eight, qkv_two, o_full = gather_weights(qkv_local[:8], qkv_local[8:], o_local)
    order = gathered_experts()
    qkv_order = np.concatenate(
        [
            (order[:, None] * 10 + np.arange(8)[None, :]).reshape(-1),
            (order[:, None] * 10 + np.arange(8, 10)[None, :]).reshape(-1),
        ]
    ).astype(np.int32)
    o_order = (order[:, None] * 8 + np.arange(8)[None, :]).reshape(-1).astype(np.int32)
    normed = rms_scale(tokens.astype(jnp.float32), attn_gain).astype(jnp.bfloat16)
    qkv_eight = qkv_eight.reshape(-1, WIDTH)
    qkv_two = qkv_two.reshape(-1, WIDTH)
    shuffled = jnp.concatenate(
        [
            lax.dot_general(normed, w, contract_rows, preferred_element_type=jnp.float32)
            for w in (qkv_eight, qkv_two)
        ],
        axis=1,
    )
    high = lax.reduce_precision(shuffled, 8, 7)
    parts = jnp.concatenate([high, shuffled - high], axis=0).astype(jnp.bfloat16)
    width_here = q_rows + 2 * kv_rows
    unshuffle = (
        jnp.asarray(qkv_order)[:, None] == jnp.arange(width_here, dtype=jnp.int32)[None, :]
    ).astype(jnp.bfloat16)
    both = jnp.dot(parts, unshuffle, preferred_element_type=jnp.float32)
    projected = both[:tok_rows] + both[tok_rows:]
    positions = jnp.arange(tok_rows).astype(jnp.float32)
    queries = rotate(
        projected[:, :q_rows].reshape(tok_rows, heads_here, HEAD_DIM), positions
    ).astype(jnp.bfloat16)
    queries = queries.reshape(tok_rows, kv_here, repeat_count, HEAD_DIM)
    key_rows = rotate(
        projected[:, q_rows : q_rows + kv_rows].reshape(tok_rows, kv_here, HEAD_DIM), positions
    ).astype(jnp.bfloat16)
    value_rows = (
        projected[:, q_rows + kv_rows :].reshape(tok_rows, kv_here, HEAD_DIM).astype(jnp.bfloat16)
    )
    attended = attention(queries, key_rows, value_rows, segment_ids, sinks)
    shuffle = (
        jnp.arange(q_rows, dtype=jnp.int32)[:, None] == jnp.asarray(o_order)[None, :]
    ).astype(jnp.bfloat16)
    attended = jnp.dot(attended, shuffle, preferred_element_type=jnp.float32).astype(jnp.bfloat16)
    update = jnp.dot(attended, o_full.reshape(-1, WIDTH), preferred_element_type=jnp.float32)
    summed = sent_and_summed(update.astype(jnp.bfloat16), "dp", 0)
    own_rows = lax.dynamic_slice_in_dim(tokens, group_index * half_rows, half_rows, 0)
    own_choices = lax.dynamic_slice_in_dim(expert_ids, group_index * half_rows, half_rows, 0)
    residual = own_rows.astype(jnp.float32) + summed
    moe_in = rms_scale(residual, mlp_gain).astype(jnp.bfloat16)
    logits = jnp.dot(moe_in, router_weight, preferred_element_type=jnp.float32) + router_bias
    experts = router_weight.shape[1]
    gate_vals = gate_values(logits, own_choices, experts).astype(jnp.bfloat16)
    slots = slot_numbers(own_choices, experts)
    code = (own_choices // 32 * 8 + own_choices % 8) * 8 + slots
    plane = own_choices // 8 % 4
    extra = jnp.concatenate(
        [
            gate_vals,
            own_choices.astype(jnp.bfloat16),
            code.astype(jnp.bfloat16),
            plane.astype(jnp.bfloat16),
            jnp.zeros((half_rows, WIDE - WIDTH - 16), jnp.bfloat16),
        ],
        axis=1,
    )
    got = dispatch_rows(jnp.concatenate([moe_in, extra], axis=1))
    dispatched, gates = finish(got)
    dispatched = jnp.transpose(dispatched, (2, 0, 1))[None, :, None]
    gates = jnp.transpose(gates).astype(jnp.bfloat16)[None, :, None]
    return (dispatched, gates)


def solution(mesh):
    return jax.shard_map(
        on_device,
        mesh=mesh,
        in_specs=(
            P("expert", None),
            P("expert"),
            P("expert", None),
            P(),
            P("dp"),
            P(("dp", "expert"), None),
            P(("dp", "expert"), None),
            P(("dp", "expert"), None),
            P(("dp", "expert"), None),
            P(("dp", "expert"), None),
            P(("dp", "expert"), None),
            P(("dp", "expert"), None),
            P(("dp", "expert"), None),
            P(),
            P(),
            P(),
        ),
        out_specs=(P("expert", None, "dp", None, None), P("expert", None, "dp", None)),
        check_vma=False,
    )
```

```python
import jax
import jax.numpy as jnp
import numpy as np
from jax import lax
from jax.experimental import pallas as pl
from jax.experimental.pallas import tpu as pltpu
from jax.sharding import PartitionSpec as P

HEAD_DIM = 64
WINDOW = 128
WIDTH = 2880
WIDE = 2944
HALF = 1408
META = 2816
MESH = pl.DeviceIdType.MESH
GATHER_SPACE = pl.ANY
FINISH_LANES = 768

beta_one = 0.9
beta_two = 0.999
adam_step = 100
learn_rate = 0.02
adam_eps = 1e-08
norm_eps = 1e-05
rope_base = 150000.0


def adam_weights(master, moment, second_mom, gradient):
    moment_new = beta_one * moment + (1.0 - beta_one) * gradient
    second_new = beta_two * second_mom + (1.0 - beta_two) * gradient * gradient
    fix_one = 1.0 - beta_one**adam_step
    fix_two = 1.0 - beta_two**adam_step
    update = moment_new / fix_one / (jnp.sqrt(second_new / fix_two) + adam_eps)
    return (master - learn_rate * update).astype(jnp.bfloat16)


def place():
    e = lax.axis_index("expert")
    core = lax.rem(e, 2)
    x = lax.rem(lax.div(e, 2), 4)
    z = lax.rem(lax.div(e, 8), 4)
    y = lax.div(e, 32)
    return e, y, z, x, core


def expert_at(y, z, x, core):
    return y * 32 + z * 8 + x * 2 + core


def step(position, by):
    return lax.rem(position + by, 4)


def greet(peers):
    barrier = pltpu.get_barrier_semaphore()
    for peer in peers:
        pl.semaphore_signal(barrier, inc=1, device_id={"expert": peer}, device_id_type=MESH)
    pl.semaphore_wait(barrier, len(peers))


def remote(src, dst, send_sem, recv_sem, peer):
    return pltpu.make_async_remote_copy(
        src_ref=src,
        dst_ref=dst,
        send_sem=send_sem,
        recv_sem=recv_sem,
        device_id={"expert": peer},
        device_id_type=MESH,
    )


def gather_kernel(a, b, o, ga, gb, go, send, recv, local):
    _, y, z, x, core = place()
    middle = y * (1 - core) + x * core
    last = x * (1 - core) + y * core

    def peer(last_at, middle_at, z_at):
        return expert_at(
            middle_at * (1 - core) + last_at * core,
            z_at,
            last_at * (1 - core) + middle_at * core,
            core,
        )

    partner = expert_at(y, z, x, 1 - core)
    ring = [
        (peer(last, middle, step(z, 1)), peer(last, middle, step(z, 3))),
        (peer(last, step(middle, 1), z), peer(last, step(middle, 3), z)),
        (peer(step(last, 1), middle, z), peer(step(last, 3), middle, z)),
    ]
    greet([p for pair in ring for p in pair] + [partner])
    streams = ((a, ga), (b, gb), (o, go))
    copies = {}

    def move(s, tag, src, dst, to):
        k = sum(1 for key in copies if key[0] == s)
        copy = remote(src, dst, send.at[s, k], recv.at[s, k], to)
        copy.start()
        copies[s, tag] = copy

    def arrived(s, tag):
        copies[s, tag].wait_recv()

    fine = ((0, 0, 4), (3, 0, 4), (1, 0, 4), (2, 0, 2), (2, 2, 2))
    coarse = (None,)
    pieces = (fine, coarse, fine)

    def part(s, last_by, k):
        full = streams[s][1]
        piece = pieces[s][k]
        if piece is None:
            return full.at[core, step(last, last_by)]
        return full.at[core, step(last, last_by), step(middle, piece[0]), pl.ds(piece[1], piece[2])]

    def along_last(s, k):
        block = part(s, 0, k)
        move(s, ("last", k, 0), block, block, ring[2][0])
        move(s, ("last", k, 1), block, block, ring[2][1])
        move(s, ("pair", 0, k), block, block, partner)

    def from_last(s, k):
        count = len(pieces[s])
        low, high = part(s, 3, k), part(s, 1, k)
        arrived(s, ("last", k, 0))
        if k < 2 and count > 1:
            move(s, ("far", k), low, low, ring[2][0])
        move(s, ("pair", 3, k), low, low, partner)
        arrived(s, ("last", k, 1))
        if k >= 2 or count == 1:
            move(s, ("far", k), high, high, ring[2][1])
        move(s, ("pair", 1, k), high, high, partner)

    own = []
    for s, (shard, full) in enumerate(streams):
        mine = full.at[core, last, middle, z]
        move(s, "z up", shard, mine, ring[0][0])
        move(s, "z down", shard, mine, ring[0][1])
        copy = pltpu.make_async_copy(shard, mine, local.at[s])
        copy.start()
        own.append(copy)
    for s, (_, full) in enumerate(streams):
        if s < 2:
            arrived(s, "z up")
            block = full.at[core, last, middle, step(z, 3)]
            move(s, "z far", block, block, ring[0][0])
        else:
            arrived(s, "z down")
            block = full.at[core, last, middle, step(z, 1)]
            move(s, "z far", block, block, ring[0][1])
    for s, (_, full) in enumerate(streams):
        arrived(s, "z down" if s < 2 else "z up")
        arrived(s, "z far")
        own[s].wait()
        block = full.at[core, last, middle]
        move(s, "middle up", block, block, ring[1][0])
        move(s, "middle down", block, block, ring[1][1])
        if s != 1:
            along_last(s, 0)
    for s, (_, full) in enumerate(streams):
        arrived(s, "middle up")
        block = full.at[core, last, step(middle, 3), pl.ds(0, 2)]
        move(s, "middle far 0", block, block, ring[1][0])
        if s != 1:
            along_last(s, 1)
        arrived(s, "middle down")
        block = full.at[core, last, step(middle, 1), pl.ds(2, 2)]
        move(s, "middle far 1", block, block, ring[1][1])
        if s != 1:
            along_last(s, 2)
    for s in range(3):
        arrived(s, "middle far 0")
        if s != 1:
            along_last(s, 3)
        arrived(s, "middle far 1")
        along_last(s, 4 if s != 1 else 0)
    for k in range(5):
        for s in range(3):
            if k < len(pieces[s]):
                from_last(s, k)
    for k in range(5):
        for s in range(3):
            if k < len(pieces[s]):
                block = part(s, 2, k)
                arrived(s, ("far", k))
                move(s, ("pair", 2, k), block, block, partner)
    for (s, tag), copy in copies.items():
        if tag[0] == "pair":
            copy.wait_recv()
    for copy in copies.values():
        copy.wait_send()


def gather_weights(a, b, o):
    return pl.pallas_call(
        gather_kernel,
        out_shape=[
            jax.ShapeDtypeStruct((2, 4, 4, 4) + v.shape, jnp.bfloat16) for v in (a, b, o)
        ],
        in_specs=[pl.BlockSpec(memory_space=pltpu.VMEM)] * 3,
        out_specs=[pl.BlockSpec(memory_space=GATHER_SPACE)] * 3,
        scratch_shapes=[
            pltpu.SemaphoreType.DMA((3, 42)),
            pltpu.SemaphoreType.DMA((3, 42)),
            pltpu.SemaphoreType.DMA((3,)),
        ],
        compiler_params=pltpu.CompilerParams(collective_id=0, has_side_effects=True),
        name="gather_weights",
    )(a, b, o)


def gathered_experts():
    core, last, middle, z = np.meshgrid(
        np.arange(2), np.arange(4), np.arange(4), np.arange(4), indexing="ij"
    )
    y = np.where(core == 0, middle, last)
    x = np.where(core == 0, last, middle)
    return (((y * 4 + z) * 4 + x) * 2 + core).reshape(-1)


PARTS = ((0, 768), (768, 768), (1536, 768), (2304, 640))


def close_kernel(
    heads,
    o_full,
    tokens_t,
    ids,
    router,
    bias,
    gain,
    got,
    rows,
    total,
    partial,
    landed,
    ring_rows,
    payload,
    picks,
    psend,
    precv,
    zsend,
    zrecv,
    send_sem,
    recv_sem,
):
    e, y, z, x, core = place()
    group = lax.axis_index("dp")
    here = y * 8 + x * 2 + core
    above, below = expert_at(y, step(z, 1), x, core), expert_at(y, step(z, 3), x, core)

    def plane_expert(index):
        return lax.div(index, 8) * 32 + z * 8 + lax.rem(index, 8)

    barrier = pltpu.get_barrier_semaphore()
    other = {"dp": 1 - group, "expert": e}
    pl.semaphore_signal(barrier, inc=1, device_id=other, device_id_type=MESH)
    for peer in (above, below):
        pl.semaphore_signal(barrier, inc=1, device_id={"expert": peer}, device_id_type=MESH)

    def signal_one(i, carry):
        peer = plane_expert(lax.rem(here + i, 32))
        pl.semaphore_signal(barrier, inc=1, device_id={"expert": peer}, device_id_type=MESH)
        return carry

    lax.fori_loop(1, 32, signal_one, 0)
    pl.semaphore_wait(barrier, 34)

    block, tail_tile = 128, pl.ds(META, 128)
    mine = pl.ds(pl.multiple_of(group * block, block), block)
    theirs = pl.ds(pl.multiple_of((1 - group) * block, block), block)
    partial[:, tail_tile] = jnp.zeros((block, 128), jnp.bfloat16)
    total[:, tail_tile] = jnp.zeros((block, 128), jnp.float32)
    exchanges = []
    for n, (start, lanes_here) in enumerate(PARTS):
        inside = pl.ds(start, min(lanes_here, WIDTH - start))
        update = jnp.dot(heads[theirs, :], o_full[:, inside], preferred_element_type=jnp.float32)
        partial[:, inside] = update.astype(jnp.bfloat16)
        lanes = pl.ds(start, lanes_here)
        copy = pltpu.make_async_remote_copy(
            src_ref=partial.at[:, lanes],
            dst_ref=landed.at[:, lanes],
            send_sem=psend.at[n],
            recv_sem=precv.at[n],
            device_id=other,
            device_id_type=MESH,
        )
        copy.start()
        exchanges.append(copy)
    for start, lanes_here in PARTS:
        inside = pl.ds(start, min(lanes_here, WIDTH - start))
        total[:, inside] = jnp.dot(
            heads[mine, :], o_full[:, inside], preferred_element_type=jnp.float32
        )
    for start in range(0, WIDTH, 128):
        inside = pl.ds(start, min(128, WIDTH - start))
        total[:, inside] = total[:, inside] + tokens_t[inside, mine].astype(jnp.float32).T

    number = lax.broadcasted_iota(jnp.int32, (block, 128), 1)
    row_number = lax.broadcasted_iota(jnp.int32, (block, 128), 0)
    choices = ids[mine, :]
    chosen = [(choices[:, k : k + 1] == number).astype(jnp.float32) for k in range(4)]
    named = (chosen[0] + chosen[1] + chosen[2] + chosen[3]).astype(jnp.bfloat16)
    earlier = jnp.dot(
        (number < row_number).astype(jnp.bfloat16), named, preferred_element_type=jnp.float32
    )
    extra = jnp.zeros((block, 128), jnp.float32)
    for k in range(4):
        pick = choices[:, k : k + 1]
        slot = jnp.sum(chosen[k] * earlier, axis=1, keepdims=True)
        code = ((pick >> 5) * 64 + (pick & 7) * 8).astype(jnp.float32) + slot
        extra = jnp.where(number == 68 + k, pick.astype(jnp.float32), extra)
        extra = jnp.where(number == 72 + k, code, extra)
        extra = jnp.where(number == 76 + k, ((pick >> 3) & 3).astype(jnp.float32), extra)

    square = jnp.zeros((block, 1), jnp.float32)
    for copy, (start, lanes_here) in zip(exchanges, PARTS):
        copy.wait_recv()
        lanes = pl.ds(start, lanes_here)
        residual = total[:, lanes] + landed[:, lanes].astype(jnp.float32)
        total[:, lanes] = residual
        square = square + jnp.sum(residual * residual, axis=1, keepdims=True)
    scale = lax.rsqrt(square * (1.0 / WIDTH) + norm_eps)
    logits = bias[...] + jnp.zeros((block, 128), jnp.float32)
    for start, lanes_here in PARTS:
        lanes = pl.ds(start, lanes_here)
        inside = pl.ds(start, min(lanes_here, WIDTH - start))
        rows[:, lanes] = (total[:, lanes] * scale * gain[:, lanes]).astype(jnp.bfloat16)
        logits = logits + jnp.dot(
            rows[:, inside], router[inside, :], preferred_element_type=jnp.float32
        )
    raised = [
        jnp.exp(jnp.sum(jnp.where(chosen[k] > 0.0, logits, 0.0), axis=1, keepdims=True))
        for k in range(4)
    ]
    norm = raised[0] + raised[1] + raised[2] + raised[3]
    for k in range(4):
        extra = jnp.where(number == 64 + k, raised[k] / norm, extra)
    rows[:, tail_tile] = rows[:, tail_tile] + extra.astype(jnp.bfloat16)

    meta = pl.ds(META, 128)
    chunks = ((0, 768), (768, 768), (1536, 768), (2304, 512))
    from_low, from_high, from_far = ring_rows.at[0], ring_rows.at[1], ring_rows.at[2]

    def pass_on(k, src, slot, lanes, peer):
        copy = remote(
            src.at[:, lanes], ring_rows.at[slot, :, lanes], zsend.at[k], zrecv.at[k], peer
        )
        copy.start()
        return copy

    def leg(n):
        if n < 4:
            up = pass_on(2 * n, rows, 0, pl.ds(*chunks[n]), above)
            down = pass_on(2 * n + 1, rows, 1, pl.ds(*chunks[3 - n]), below)
        else:
            up = pass_on(2 * n, from_low, 2, pl.ds(*chunks[n - 4]), above)
            down = pass_on(2 * n + 1, from_high, 2, pl.ds(*chunks[7 - n]), below)
        return up, down

    low_meta = pass_on(12, rows, 0, meta, above)
    high_meta = pass_on(13, rows, 1, meta, below)
    legs = [leg(0)]

    def choose(block, source):
        data = source[:, META:WIDE].astype(jnp.float32)
        code = lax.broadcasted_iota(jnp.int32, (128, 256), 1).astype(jnp.float32)
        plane = z.astype(jnp.float32)
        hit = jnp.zeros((128, 256), jnp.float32)
        for k in range(4):
            same = (data[:, 72 + k : 73 + k] == code) & (data[:, 76 + k : 77 + k] == plane)
            hit = hit + jnp.where(same, 1.0, 0.0)
        picks[block] = hit.T.astype(jnp.bfloat16)

    def deliver(block, source, z_at, chunk):
        start, lanes_here = chunks[chunk]
        lanes_here = lanes_here if chunk < 3 else WIDE - start
        for at in range(0, lanes_here, 384):
            lanes = pl.ds(start + at, min(384, lanes_here - at))
            slots = jnp.dot(picks[block], source[:, lanes], preferred_element_type=jnp.float32)
            payload[block, :, :, lanes] = slots.reshape(32, 8, -1).astype(jnp.bfloat16)
        lanes = pl.ds(start, lanes_here)
        row = expert_at(y, z_at, x, core)
        pltpu.make_async_copy(
            payload.at[block, here, :, lanes], got.at[row, :, lanes], recv_sem
        ).start()

        def one(i, carry):
            index = lax.rem(here + i, 32)
            remote(
                payload.at[block, index, :, lanes],
                got.at[row, :, lanes],
                send_sem,
                recv_sem,
                plane_expert(index),
            ).start()
            return carry

        lax.fori_loop(1, 32, one, 0)

    choose(0, rows)
    for chunk in range(4):
        deliver(0, rows, z, chunk)
    low_meta.wait_recv()
    far_meta = pass_on(14, from_low, 2, meta, above)
    high_meta.wait_recv()
    choose(1, from_low)
    choose(2, from_high)
    for n in range(6):
        up, down = legs[n]
        if n < 5:
            up.wait_send()
            down.wait_send()
            legs.append(leg(n + 1))
        if n == 3:
            far_meta.wait_recv()
            choose(3, from_far)
        up.wait_recv()
        deliver(*((1, from_low, step(z, 3), n) if n < 4 else (3, from_far, step(z, 2), n - 4)))
        down.wait_recv()
        deliver(*((2, from_high, step(z, 1), 3 - n) if n < 4 else (3, from_far, step(z, 2), 7 - n)))
    pltpu.make_async_copy(got, got, recv_sem).wait()
    part = payload.at[:, pl.ds(0, 31)]
    pltpu.make_async_copy(part, part, send_sem).wait()
    for copy in (low_meta, high_meta, far_meta, *legs[5], *exchanges):
        copy.wait_send()


def close(heads, o_full, tokens_t, ids, router, bias, gain):
    return pl.pallas_call(
        close_kernel,
        out_shape=jax.ShapeDtypeStruct((128, 8, WIDE), jnp.bfloat16),
        in_specs=[pl.BlockSpec(memory_space=pltpu.VMEM)] * 7,
        out_specs=pl.BlockSpec(memory_space=pl.ANY),
        scratch_shapes=[
            pltpu.VMEM((128, WIDE), jnp.bfloat16),
            pltpu.VMEM((128, WIDE), jnp.float32),
            pltpu.VMEM((128, WIDE), jnp.bfloat16),
            pltpu.VMEM((128, WIDE), jnp.bfloat16),
            pltpu.VMEM((3, 128, WIDE), jnp.bfloat16),
            pltpu.VMEM((4, 32, 8, WIDE), jnp.bfloat16),
            pltpu.VMEM((4, 256, 128), jnp.bfloat16),
            pltpu.SemaphoreType.DMA((4,)),
            pltpu.SemaphoreType.DMA((4,)),
            pltpu.SemaphoreType.DMA((15,)),
            pltpu.SemaphoreType.DMA((15,)),
            pltpu.SemaphoreType.DMA,
            pltpu.SemaphoreType.DMA,
        ],
        compiler_params=pltpu.CompilerParams(
            collective_id=1, has_side_effects=True, vmem_limit_bytes=60 * 1024 * 1024
        ),
        name="close",
    )(heads, o_full, tokens_t, ids, router, bias, gain)


def attend_kernel(
    qkv_eight,
    qkv_two,
    tokens_t,
    gain,
    segments,
    sinks,
    cosine,
    sine,
    heads,
    weights,
    normed,
    from_eight,
    from_two,
    projected,
    attended,
    sem,
):
    fetch = pltpu.make_async_copy(qkv_eight, weights, sem)
    fetch.start()
    order = gathered_experts()
    square = jnp.zeros((1, 256), jnp.float32)
    for start in range(0, WIDTH, 192):
        chunk = tokens_t[start : start + 192].astype(jnp.float32)
        square = square + jnp.sum(chunk * chunk, axis=0, keepdims=True)
    scale = lax.rsqrt(square * (1.0 / WIDTH) + norm_eps)
    for start in range(0, WIDTH, 128):
        size = min(128, WIDTH - start)
        column = jnp.broadcast_to(gain[:, start : start + size], (128, size)).T
        for half in range(2):
            lanes = slice(half * 128, half * 128 + 128)
            chunk = tokens_t[start : start + size, lanes].astype(jnp.float32)
            normed[start : start + size, lanes] = (chunk * scale[:, lanes] * column).astype(
                jnp.bfloat16
            )
    from_two[...] = jnp.dot(qkv_two[...], normed[...], preferred_element_type=jnp.float32)
    fetch.wait()
    for start in range(0, 1024, 256):
        from_eight[start : start + 256] = jnp.dot(
            weights[start : start + 256], normed[...], preferred_element_type=jnp.float32
        )
    for g in range(128):
        row = int(order[g]) * 10
        projected[row : row + 8] = from_eight[g * 8 : g * 8 + 8]
        projected[row + 8 : row + 10] = from_two[g * 2 : g * 2 + 2]

    def turn(row):
        first, second = projected[row : row + 32], projected[row + 32 : row + 64]
        return jnp.concatenate(
            [
                first * cosine[...] - second * sine[...],
                second * cosine[...] + first * sine[...],
            ],
            axis=0,
        )

    owner = segments[...]
    other = jnp.concatenate(
        [jnp.broadcast_to(owner[:, h * 128 : h * 128 + 128], (128, 128)).T for h in range(2)], axis=0
    )
    other = jnp.concatenate([other, other], axis=1)
    behind = lax.broadcasted_iota(jnp.int32, (256, 256), 1) - lax.broadcasted_iota(
        jnp.int32, (256, 256), 0
    )
    allowed = (other == owner) & (behind >= 0) & (behind < WINDOW)
    allowed = allowed.astype(jnp.float32)
    for kv in range(2):
        keys = turn(1024 + kv * 64).T.astype(jnp.bfloat16)
        values = projected[1152 + kv * 64 : 1216 + kv * 64].astype(jnp.bfloat16)
        for h in range(kv * 8, kv * 8 + 8):
            queries = turn(h * 64).astype(jnp.bfloat16)
            scores = jnp.dot(keys, queries, preferred_element_type=jnp.float32)
            shares = jnp.where(allowed > 0.0, jnp.exp(scores * HEAD_DIM**-0.5), 0.0)
            running = jnp.exp(sinks[:, h : h + 1]) + jnp.sum(shares, axis=0, keepdims=True)
            probs = (shares * (1.0 / running)).astype(jnp.bfloat16)
            attended[h * 64 : h * 64 + 64] = jnp.dot(
                values, probs, preferred_element_type=jnp.float32
            )
    for j in range(8):
        cut = jnp.concatenate(
            [
                attended[int(order[g]) * 8 : int(order[g]) * 8 + 8]
                for g in range(j * 16, j * 16 + 16)
            ],
            axis=0,
        )
        for half in range(2):
            heads[half * 128 : half * 128 + 128, j * 128 : j * 128 + 128] = (
                cut[:, half * 128 : half * 128 + 128].T.astype(jnp.bfloat16)
            )


def attend(qkv_eight, qkv_two, tokens_t, gain, segments, sinks, cosine, sine):
    return pl.pallas_call(
        attend_kernel,
        out_shape=jax.ShapeDtypeStruct((256, 1024), jnp.bfloat16),
        in_specs=[pl.BlockSpec(memory_space=pl.ANY)]
        + [pl.BlockSpec(memory_space=pltpu.VMEM)] * 7,
        out_specs=pl.BlockSpec(memory_space=pltpu.VMEM),
        scratch_shapes=[
            pltpu.VMEM((1024, WIDTH), jnp.bfloat16),
            pltpu.VMEM((WIDTH, 256), jnp.bfloat16),
            pltpu.VMEM((1024, 256), jnp.float32),
            pltpu.VMEM((256, 256), jnp.float32),
            pltpu.VMEM((1280, 256), jnp.float32),
            pltpu.VMEM((1024, 256), jnp.float32),
            pltpu.SemaphoreType.DMA,
        ],
        compiler_params=pltpu.CompilerParams(vmem_limit_bytes=48 * 1024 * 1024),
        name="attend",
    )(qkv_eight, qkv_two, tokens_t, gain, segments, sinks, cosine, sine)


def finish_kernel(got, out, gates):
    spot = pl.program_id(0)
    lanes_here = got.shape[2]
    halves = []
    for part in range(2):
        rows = got[part * 64 : part * 64 + 64].reshape(512, lanes_here)
        source = lax.broadcasted_iota(jnp.int32, (512, 512), 0)
        target = lax.broadcasted_iota(jnp.int32, (512, 512), 1)
        pick = (source == (target & 63) * 8 + (target >> 6)).astype(jnp.bfloat16)
        halves.append(
            lax.dot_general(rows, pick, (((0,), (0,)), ((), ())), preferred_element_type=jnp.float32)
        )
    whole = []
    for c in range(8):
        cut = slice(c * 64, c * 64 + 64)
        whole.append(jnp.concatenate([halves[0][:, cut], halves[1][:, cut]], axis=1))
        out[c] = whole[c].astype(jnp.bfloat16)

    @pl.when(spot == WIDTH // FINISH_LANES)
    def _():
        mine = lax.axis_index("expert").astype(jnp.float32)
        first = WIDTH % FINISH_LANES
        for c in range(8):
            data = whole[c][first : first + 8]
            asked = jnp.where(data[4:8] == mine, data[:4], 0.0)
            gates[c : c + 1] = jnp.sum(asked, axis=0, keepdims=True)


def finish(got):
    return pl.pallas_call(
        finish_kernel,
        grid=(-(-WIDE // FINISH_LANES),),
        out_shape=[
            jax.ShapeDtypeStruct((8, WIDTH, 128), jnp.bfloat16),
            jax.ShapeDtypeStruct((8, 128), jnp.float32),
        ],
        in_specs=[pl.BlockSpec((128, 8, FINISH_LANES), lambda i: (0, 0, i))],
        out_specs=[
            pl.BlockSpec((8, FINISH_LANES, 128), lambda i: (0, i, 0)),
            pl.BlockSpec((8, 128), lambda i: (0, 0)),
        ],
        name="finish",
    )(got)


def on_device(
    tokens,
    segment_ids,
    expert_ids,
    attn_gain,
    sinks,
    qkv_master,
    qkv_mom,
    qkv_var,
    qkv_grad,
    o_master,
    o_mom,
    o_var,
    o_grad,
    router_weight,
    router_bias,
    mlp_gain,
):
    tok_rows = tokens.shape[0]
    qkv_local = adam_weights(qkv_master, qkv_mom, qkv_var, qkv_grad)
    o_local = adam_weights(o_master, o_mom, o_var, o_grad)
    qkv_eight, qkv_two, o_full = gather_weights(qkv_local[:8], qkv_local[8:], o_local)
    positions = jnp.arange(tok_rows).astype(jnp.float32)
    spread = jnp.arange(HEAD_DIM // 2).astype(jnp.float32) * 2.0 / HEAD_DIM
    angles = (rope_base**-spread)[:, None] * positions[None, :]
    heads = attend(
        qkv_eight.reshape(-1, WIDTH),
        qkv_two.reshape(-1, WIDTH),
        tokens.T,
        attn_gain[None, :],
        segment_ids.astype(jnp.float32)[None, :],
        sinks[None, :],
        jnp.cos(angles),
        jnp.sin(angles),
    )
    got = close(
        heads,
        o_full.reshape(-1, WIDTH),
        tokens.T,
        expert_ids,
        router_weight,
        router_bias[None, :],
        jnp.pad(mlp_gain, (0, WIDE - WIDTH))[None, :],
    )
    dispatched, gates = finish(got)
    dispatched = jnp.transpose(dispatched, (2, 0, 1))[None, :, None]
    gates = jnp.transpose(gates).astype(jnp.bfloat16)[None, :, None]
    return (dispatched, gates)


def solution(mesh):
    return jax.shard_map(
        on_device,
        mesh=mesh,
        in_specs=(
            P("expert", None),
            P("expert"),
            P("expert", None),
            P(),
            P("dp"),
            P(("dp", "expert"), None),
            P(("dp", "expert"), None),
            P(("dp", "expert"), None),
            P(("dp", "expert"), None),
            P(("dp", "expert"), None),
            P(("dp", "expert"), None),
            P(("dp", "expert"), None),
            P(("dp", "expert"), None),
            P(),
            P(),
            P(),
        ),
        out_specs=(P("expert", None, "dp", None, None), P("expert", None, "dp", None)),
        check_vma=False,
    )
```

```python
import jax
import jax.numpy as jnp
import numpy as np
from jax import lax
from jax.experimental import pallas as pl
from jax.experimental.pallas import tpu as pltpu
from jax.sharding import PartitionSpec as P

HEAD_DIM = 64
WINDOW = 128
WIDTH = 2880
WIDE = 2944
HALF = 1408
META = 2816
MESH = pl.DeviceIdType.MESH
FINISH_LANES = 768

beta_one = 0.9
beta_two = 0.999
adam_step = 100
learn_rate = 0.02
adam_eps = 1e-08
norm_eps = 1e-05
rope_base = 150000.0


def adam_weights(master, moment, second_mom, gradient):
    moment_new = beta_one * moment + (1.0 - beta_one) * gradient
    second_new = beta_two * second_mom + (1.0 - beta_two) * gradient * gradient
    fix_one = 1.0 - beta_one**adam_step
    fix_two = 1.0 - beta_two**adam_step
    update = moment_new / fix_one / (jnp.sqrt(second_new / fix_two) + adam_eps)
    return (master - learn_rate * update).astype(jnp.bfloat16)


def place():
    e = lax.axis_index("expert")
    core = lax.rem(e, 2)
    x = lax.rem(lax.div(e, 2), 4)
    z = lax.rem(lax.div(e, 8), 4)
    y = lax.div(e, 32)
    return e, y, z, x, core


def expert_at(y, z, x, core):
    return y * 32 + z * 8 + x * 2 + core


def step(position, by):
    return lax.rem(position + by, 4)


def greet(peers):
    barrier = pltpu.get_barrier_semaphore()
    for peer in peers:
        pl.semaphore_signal(barrier, inc=1, device_id={"expert": peer}, device_id_type=MESH)
    pl.semaphore_wait(barrier, len(peers))


def remote(src, dst, send_sem, recv_sem, peer):
    return pltpu.make_async_remote_copy(
        src_ref=src,
        dst_ref=dst,
        send_sem=send_sem,
        recv_sem=recv_sem,
        device_id={"expert": peer},
        device_id_type=MESH,
    )


def gathered_experts():
    core, last, middle, z = np.meshgrid(
        np.arange(2), np.arange(4), np.arange(4), np.arange(4), indexing="ij"
    )
    y = np.where(core == 0, middle, last)
    x = np.where(core == 0, last, middle)
    return (((y * 4 + z) * 4 + x) * 2 + core).reshape(-1)


def open_kernel(
    a,
    b,
    o,
    tokens,
    gain,
    segments,
    sinks,
    cosine,
    sine,
    go,
    heads,
    tokens_t,
    ga,
    gb,
    normed,
    from_eight,
    from_two,
    two_rows,
    projected,
    attended,
    send,
    recv,
    local,
):
    _, y, z, x, core = place()
    middle = y * (1 - core) + x * core
    last = x * (1 - core) + y * core

    def peer(last_at, middle_at, z_at):
        return expert_at(
            middle_at * (1 - core) + last_at * core,
            z_at,
            last_at * (1 - core) + middle_at * core,
            core,
        )

    partner = expert_at(y, z, x, 1 - core)
    ring = [
        (peer(last, middle, step(z, 1)), peer(last, middle, step(z, 3))),
        (peer(last, step(middle, 1), z), peer(last, step(middle, 3), z)),
        (peer(step(last, 1), middle, z), peer(step(last, 3), middle, z)),
    ]
    greet([p for pair in ring for p in pair] + [partner])
    streams = ((a, ga), (b, gb), (o, go))
    copies = {}
    fetch = pltpu.make_async_copy(tokens, tokens_t, local.at[3])
    fetch.start()

    def move(s, tag, src, dst, to):
        k = sum(1 for key in copies if key[0] == s)
        copy = remote(src, dst, send.at[s, k], recv.at[s, k], to)
        copy.start()
        copies[s, tag] = copy

    def arrived(s, tag):
        copies[s, tag].wait_recv()

    fine = ((0, 0, 4), (3, 0, 4), (1, 0, 4), (2, 0, 2), (2, 2, 2))
    coarse = (None,)
    pieces = (fine, coarse, fine)

    def part(s, last_by, k):
        full = streams[s][1]
        piece = pieces[s][k]
        if piece is None:
            return full.at[core, step(last, last_by)]
        return full.at[core, step(last, last_by), step(middle, piece[0]), pl.ds(piece[1], piece[2])]

    def along_last(s, k):
        block = part(s, 0, k)
        move(s, ("last", k, 0), block, block, ring[2][0])
        move(s, ("last", k, 1), block, block, ring[2][1])
        move(s, ("pair", 0, k), block, block, partner)

    def from_last(s, k):
        count = len(pieces[s])
        low, high = part(s, 3, k), part(s, 1, k)
        arrived(s, ("last", k, 0))
        if k < 2 and count > 1:
            move(s, ("far", k), low, low, ring[2][0])
        move(s, ("pair", 3, k), low, low, partner)
        arrived(s, ("last", k, 1))
        if k >= 2 or count == 1:
            move(s, ("far", k), high, high, ring[2][1])
        move(s, ("pair", 1, k), high, high, partner)

    own = []
    for s, (shard, full) in enumerate(streams):
        mine = full.at[core, last, middle, z]
        move(s, "z up", shard, mine, ring[0][0])
        move(s, "z down", shard, mine, ring[0][1])
        copy = pltpu.make_async_copy(shard, mine, local.at[s])
        copy.start()
        own.append(copy)
    for s, (_, full) in enumerate(streams):
        if s < 2:
            arrived(s, "z up")
            block = full.at[core, last, middle, step(z, 3)]
            move(s, "z far", block, block, ring[0][0])
        else:
            arrived(s, "z down")
            block = full.at[core, last, middle, step(z, 1)]
            move(s, "z far", block, block, ring[0][1])
    for s, (_, full) in enumerate(streams):
        arrived(s, "z down" if s < 2 else "z up")
        arrived(s, "z far")
        own[s].wait()
        block = full.at[core, last, middle]
        move(s, "middle up", block, block, ring[1][0])
        move(s, "middle down", block, block, ring[1][1])
        if s == 0:
            along_last(s, 0)
    for s, (_, full) in enumerate(streams):
        arrived(s, "middle up")
        block = full.at[core, last, step(middle, 3), pl.ds(0, 2)]
        move(s, "middle far 0", block, block, ring[1][0])
        if s == 0:
            along_last(s, 1)
        arrived(s, "middle down")
        block = full.at[core, last, step(middle, 1), pl.ds(2, 2)]
        move(s, "middle far 1", block, block, ring[1][1])
        if s == 0:
            along_last(s, 2)
    for s in range(3):
        arrived(s, "middle far 0")
        if s == 0:
            along_last(s, 3)
        arrived(s, "middle far 1")
        if s < 2:
            along_last(s, 4 if s == 0 else 0)
    fetch.wait()
    square = jnp.zeros((1, 256), jnp.float32)
    for start in range(0, WIDTH, 192):
        chunk = tokens_t[start : start + 192].astype(jnp.float32)
        square = square + jnp.sum(chunk * chunk, axis=0, keepdims=True)
    scale = lax.rsqrt(square * (1.0 / WIDTH) + norm_eps)
    for start in range(0, WIDTH, 128):
        size = min(128, WIDTH - start)
        column = jnp.broadcast_to(gain[0:1, start : start + size], (128, size)).T
        for half in range(2):
            lanes = slice(half * 128, half * 128 + 128)
            chunk = tokens_t[start : start + size, lanes].astype(jnp.float32)
            normed[start : start + size, lanes] = (chunk * scale[:, lanes] * column).astype(
                jnp.bfloat16
            )
    for k in range(5):
        from_last(0, k)
        if k == 0:
            from_last(1, 0)
        if k >= 2:
            along_last(2, k - 2)
    along_last(2, 3)
    along_last(2, 4)

    def from_far(s, k):
        block = part(s, 2, k)
        arrived(s, ("far", k))
        move(s, ("pair", 2, k), block, block, partner)

    for k in range(5):
        from_far(0, k)
    from_far(1, 0)

    def output_step(n):
        if n < 5:
            from_last(2, n)
        elif n < 10:
            from_far(2, n - 5)

    for (s, tag), copy in copies.items():
        if s < 2 and tag[0] == "pair":
            copy.wait_recv()
    output_step(0)
    order = gathered_experts()
    for n in range(128):
        two = gb[n // 64, n // 16 % 4, n // 4 % 4, n % 4]
        two_rows[n * 2 : n * 2 + 2] = two.astype(jnp.float32)
    output_step(1)
    from_two[...] = jnp.dot(
        two_rows[...].astype(jnp.bfloat16), normed[...], preferred_element_type=jnp.float32
    )
    for n in range(4):
        rows = ga[n // 2, n % 2 * 2 : n % 2 * 2 + 2].reshape(256, WIDTH)
        from_eight[n * 256 : n * 256 + 256] = jnp.dot(
            rows, normed[...], preferred_element_type=jnp.float32
        )
        if n % 2 == 1:
            output_step(2 + n // 2)
    for g in range(128):
        row = int(order[g]) * 10
        projected[row : row + 8] = from_eight[g * 8 : g * 8 + 8]
        projected[row + 8 : row + 10] = from_two[g * 2 : g * 2 + 2]
    output_step(4)

    def turn(row):
        first, second = projected[row : row + 32], projected[row + 32 : row + 64]
        return jnp.concatenate(
            [
                first * cosine[...] - second * sine[...],
                second * cosine[...] + first * sine[...],
            ],
            axis=0,
        )

    owner = segments[...].astype(jnp.float32)
    other = jnp.concatenate(
        [jnp.broadcast_to(owner[:, h * 128 : h * 128 + 128], (128, 128)).T for h in range(2)], axis=0
    )
    other = jnp.concatenate([other, other], axis=1)
    behind = lax.broadcasted_iota(jnp.int32, (256, 256), 1) - lax.broadcasted_iota(
        jnp.int32, (256, 256), 0
    )
    allowed = (other == owner) & (behind >= 0) & (behind < WINDOW)
    allowed = allowed.astype(jnp.float32)
    for kv in range(2):
        keys = turn(1024 + kv * 64).T.astype(jnp.bfloat16)
        values = projected[1152 + kv * 64 : 1216 + kv * 64].astype(jnp.bfloat16)
        for h in range(kv * 8, kv * 8 + 8):
            if h % 4 == 0:
                output_step(h // 4 + 5)
            queries = turn(h * 64).astype(jnp.bfloat16)
            scores = jnp.dot(keys, queries, preferred_element_type=jnp.float32)
            shares = jnp.where(allowed > 0.0, jnp.exp(scores * HEAD_DIM**-0.5), 0.0)
            running = jnp.exp(sinks[:, h : h + 1]) + jnp.sum(shares, axis=0, keepdims=True)
            probs = (shares * (1.0 / running)).astype(jnp.bfloat16)
            attended[h * 64 : h * 64 + 64] = jnp.dot(
                values, probs, preferred_element_type=jnp.float32
            )
    output_step(9)
    for j in range(8):
        cut = jnp.concatenate(
            [
                attended[int(order[g]) * 8 : int(order[g]) * 8 + 8]
                for g in range(j * 16, j * 16 + 16)
            ],
            axis=0,
        )
        for half in range(2):
            heads[half * 128 : half * 128 + 128, j * 128 : j * 128 + 128] = (
                cut[:, half * 128 : half * 128 + 128].T.astype(jnp.bfloat16)
            )
    for (s, tag), copy in copies.items():
        if s == 2 and tag[0] == "pair":
            copy.wait_recv()
    for copy in copies.values():
        copy.wait_send()


def open_up(a, b, o, tokens_t, gain, segments, sinks, cosine, sine):
    return pl.pallas_call(
        open_kernel,
        out_shape=[
            jax.ShapeDtypeStruct((2, 4, 4, 4, 8, WIDTH), jnp.bfloat16),
            jax.ShapeDtypeStruct((256, 1024), jnp.bfloat16),
        ],
        in_specs=[pl.BlockSpec(memory_space=pltpu.VMEM)] * 3
        + [pl.BlockSpec(memory_space=pltpu.HBM)]
        + [pl.BlockSpec(memory_space=pltpu.VMEM)] * 5,
        out_specs=[
            pl.BlockSpec(memory_space=pl.ANY),
            pl.BlockSpec(memory_space=pltpu.VMEM),
        ],
        scratch_shapes=[
            pltpu.VMEM((WIDTH, 256), jnp.bfloat16),
            pltpu.VMEM((2, 4, 4, 4, 8, WIDTH), jnp.bfloat16),
            pltpu.VMEM((2, 4, 4, 4, 2, WIDTH), jnp.bfloat16),
            pltpu.VMEM((WIDTH, 256), jnp.bfloat16),
            pltpu.VMEM((1024, 256), jnp.float32),
            pltpu.VMEM((256, 256), jnp.float32),
            pltpu.VMEM((256, WIDTH), jnp.float32),
            pltpu.VMEM((1280, 256), jnp.float32),
            pltpu.VMEM((1024, 256), jnp.float32),
            pltpu.SemaphoreType.DMA((3, 42)),
            pltpu.SemaphoreType.DMA((3, 42)),
            pltpu.SemaphoreType.DMA((4,)),
        ],
        compiler_params=pltpu.CompilerParams(
            collective_id=0, has_side_effects=True, vmem_limit_bytes=60 * 1024 * 1024
        ),
        name="open",
    )(a, b, o, tokens_t, gain, segments, sinks, cosine, sine)


PARTS = ((0, 768), (768, 768), (1536, 768), (2304, 640))


def close_kernel(
    heads,
    o_there,
    tokens,
    ids,
    router,
    bias,
    gain,
    got,
    o_full,
    tokens_t,
    rows,
    total,
    partial,
    landed,
    ring_rows,
    payload,
    picks,
    psend,
    precv,
    zsend,
    zrecv,
    send_sem,
    recv_sem,
    local,
):
    fetches = [
        pltpu.make_async_copy(src, dst, local.at[k])
        for k, (src, dst) in enumerate(((o_there, o_full), (tokens, tokens_t)))
    ]
    for copy in fetches:
        copy.start()
    e, y, z, x, core = place()
    group = lax.axis_index("dp")
    here = y * 8 + x * 2 + core
    above, below = expert_at(y, step(z, 1), x, core), expert_at(y, step(z, 3), x, core)

    def plane_expert(index):
        return lax.div(index, 8) * 32 + z * 8 + lax.rem(index, 8)

    barrier = pltpu.get_barrier_semaphore()
    other = {"dp": 1 - group, "expert": e}
    pl.semaphore_signal(barrier, inc=1, device_id=other, device_id_type=MESH)
    for peer in (above, below):
        pl.semaphore_signal(barrier, inc=1, device_id={"expert": peer}, device_id_type=MESH)

    def signal_one(i, carry):
        peer = plane_expert(lax.rem(here + i, 32))
        pl.semaphore_signal(barrier, inc=1, device_id={"expert": peer}, device_id_type=MESH)
        return carry

    lax.fori_loop(1, 32, signal_one, 0)
    pl.semaphore_wait(barrier, 34)

    block, tail_tile = 128, pl.ds(META, 128)
    mine = pl.ds(pl.multiple_of(group * block, block), block)
    theirs = pl.ds(pl.multiple_of((1 - group) * block, block), block)
    partial[:, tail_tile] = jnp.zeros((block, 128), jnp.bfloat16)
    total[:, tail_tile] = jnp.zeros((block, 128), jnp.float32)
    exchanges = []
    fetches[0].wait()
    for n, (start, lanes_here) in enumerate(PARTS):
        inside = pl.ds(start, min(lanes_here, WIDTH - start))
        update = jnp.dot(heads[theirs, :], o_full[:, inside], preferred_element_type=jnp.float32)
        partial[:, inside] = update.astype(jnp.bfloat16)
        lanes = pl.ds(start, lanes_here)
        copy = pltpu.make_async_remote_copy(
            src_ref=partial.at[:, lanes],
            dst_ref=landed.at[:, lanes],
            send_sem=psend.at[n],
            recv_sem=precv.at[n],
            device_id=other,
            device_id_type=MESH,
        )
        copy.start()
        exchanges.append(copy)
    for start, lanes_here in PARTS:
        inside = pl.ds(start, min(lanes_here, WIDTH - start))
        total[:, inside] = jnp.dot(
            heads[mine, :], o_full[:, inside], preferred_element_type=jnp.float32
        )
    fetches[1].wait()
    for start in range(0, WIDTH, 128):
        inside = pl.ds(start, min(128, WIDTH - start))
        total[:, inside] = total[:, inside] + tokens_t[inside, mine].astype(jnp.float32).T

    number = lax.broadcasted_iota(jnp.int32, (block, 128), 1)
    row_number = lax.broadcasted_iota(jnp.int32, (block, 128), 0)
    chosen = [(ids[k : k + 1, mine] == row_number).astype(jnp.float32).T for k in range(4)]
    named = (chosen[0] + chosen[1] + chosen[2] + chosen[3]).astype(jnp.bfloat16)
    earlier = jnp.dot(
        (number < row_number).astype(jnp.bfloat16), named, preferred_element_type=jnp.float32
    )
    expert = number.astype(jnp.float32)
    first_slot = ((number >> 5) * 64 + (number & 7) * 8).astype(jnp.float32) + earlier
    plane_of = ((number >> 3) & 3).astype(jnp.float32)
    extra = jnp.zeros((block, 128), jnp.float32)
    for k in range(4):
        for at, what in ((68, expert), (72, first_slot), (76, plane_of)):
            value = jnp.sum(chosen[k] * what, axis=1, keepdims=True)
            extra = jnp.where(number == at + k, value, extra)

    square = jnp.zeros((block, 1), jnp.float32)
    for copy, (start, lanes_here) in zip(exchanges, PARTS):
        copy.wait_recv()
        lanes = pl.ds(start, lanes_here)
        residual = total[:, lanes] + landed[:, lanes].astype(jnp.float32)
        total[:, lanes] = residual
        square = square + jnp.sum(residual * residual, axis=1, keepdims=True)
    scale = lax.rsqrt(square * (1.0 / WIDTH) + norm_eps)
    logits = bias[...] + jnp.zeros((block, 128), jnp.float32)
    for start, lanes_here in PARTS:
        inside = pl.ds(start, min(lanes_here, WIDTH - start))
        rows[:, inside] = (total[:, inside] * scale * gain[:, inside]).astype(jnp.bfloat16)
        logits = logits + jnp.dot(
            rows[:, inside], router[inside, :], preferred_element_type=jnp.float32
        )
    raised = [
        jnp.exp(jnp.sum(jnp.where(chosen[k] > 0.0, logits, 0.0), axis=1, keepdims=True))
        for k in range(4)
    ]
    norm = raised[0] + raised[1] + raised[2] + raised[3]
    for k in range(4):
        extra = jnp.where(number == 64 + k, raised[k] / norm, extra)
    rows[:, tail_tile] = jnp.where(
        number < WIDTH - META, rows[:, tail_tile].astype(jnp.float32), extra
    ).astype(jnp.bfloat16)

    meta = pl.ds(META, 128)
    chunks = ((0, 768), (768, 768), (1536, 768), (2304, 512))
    from_low, from_high, from_far = ring_rows.at[0], ring_rows.at[1], ring_rows.at[2]

    def pass_on(k, src, slot, lanes, peer):
        copy = remote(
            src.at[:, lanes], ring_rows.at[slot, :, lanes], zsend.at[k], zrecv.at[k], peer
        )
        copy.start()
        return copy

    def leg(n):
        if n < 4:
            up = pass_on(2 * n, rows, 0, pl.ds(*chunks[n]), above)
            down = pass_on(2 * n + 1, rows, 1, pl.ds(*chunks[3 - n]), below)
        else:
            up = pass_on(2 * n, from_low, 2, pl.ds(*chunks[n - 4]), above)
            down = pass_on(2 * n + 1, from_high, 2, pl.ds(*chunks[7 - n]), below)
        return up, down

    low_meta = pass_on(12, rows, 0, meta, above)
    high_meta = pass_on(13, rows, 1, meta, below)
    legs = [leg(0)]

    def choose(block, source):
        data = source[:, META:WIDE].astype(jnp.float32)
        code = lax.broadcasted_iota(jnp.int32, (128, 256), 1).astype(jnp.float32)
        plane = z.astype(jnp.float32)
        hit = jnp.zeros((128, 256), jnp.float32)
        for k in range(4):
            same = (data[:, 72 + k : 73 + k] == code) & (data[:, 76 + k : 77 + k] == plane)
            hit = hit + jnp.where(same, 1.0, 0.0)
        picks[block] = hit.T.astype(jnp.bfloat16)

    def deliver(block, source, z_at, chunk):
        start, lanes_here = chunks[chunk]
        lanes_here = lanes_here if chunk < 3 else WIDE - start
        for at in range(0, lanes_here, 384):
            lanes = pl.ds(start + at, min(384, lanes_here - at))
            slots = jnp.dot(picks[block], source[:, lanes], preferred_element_type=jnp.float32)
            payload[block, :, :, lanes] = slots.reshape(32, 8, -1).astype(jnp.bfloat16)
        lanes = pl.ds(start, lanes_here)
        row = expert_at(y, z_at, x, core)
        pltpu.make_async_copy(
            payload.at[block, here, :, lanes], got.at[row, :, lanes], recv_sem
        ).start()

        def one(i, carry):
            index = lax.rem(here + i, 32)
            remote(
                payload.at[block, index, :, lanes],
                got.at[row, :, lanes],
                send_sem,
                recv_sem,
                plane_expert(index),
            ).start()
            return carry

        lax.fori_loop(1, 32, one, 0)

    choose(0, rows)
    for chunk in range(4):
        deliver(0, rows, z, chunk)
    low_meta.wait_recv()
    far_meta = pass_on(14, from_low, 2, meta, above)
    high_meta.wait_recv()
    choose(1, from_low)
    choose(2, from_high)
    for n in range(6):
        up, down = legs[n]
        if n < 5:
            up.wait_send()
            down.wait_send()
            legs.append(leg(n + 1))
        if n == 3:
            far_meta.wait_recv()
            choose(3, from_far)
        up.wait_recv()
        deliver(*((1, from_low, step(z, 3), n) if n < 4 else (3, from_far, step(z, 2), n - 4)))
        down.wait_recv()
        deliver(*((2, from_high, step(z, 1), 3 - n) if n < 4 else (3, from_far, step(z, 2), 7 - n)))
    pltpu.make_async_copy(got, got, recv_sem).wait()
    part = payload.at[:, pl.ds(0, 31)]
    pltpu.make_async_copy(part, part, send_sem).wait()
    for copy in (low_meta, high_meta, far_meta, *legs[5], *exchanges):
        copy.wait_send()


def close(heads, o_full, tokens_t, ids, router, bias, gain):
    return pl.pallas_call(
        close_kernel,
        out_shape=jax.ShapeDtypeStruct((128, 8, WIDE), jnp.bfloat16),
        in_specs=[pl.BlockSpec(memory_space=pltpu.VMEM)]
        + [pl.BlockSpec(memory_space=pltpu.HBM)] * 2
        + [pl.BlockSpec(memory_space=pltpu.VMEM)] * 4,
        out_specs=pl.BlockSpec(memory_space=pl.ANY),
        scratch_shapes=[
            pltpu.VMEM((1024, WIDTH), jnp.bfloat16),
            pltpu.VMEM((WIDTH, 256), jnp.bfloat16),
            pltpu.VMEM((128, WIDE), jnp.bfloat16),
            pltpu.VMEM((128, WIDE), jnp.float32),
            pltpu.VMEM((128, WIDE), jnp.bfloat16),
            pltpu.VMEM((128, WIDE), jnp.bfloat16),
            pltpu.VMEM((3, 128, WIDE), jnp.bfloat16),
            pltpu.VMEM((4, 32, 8, WIDE), jnp.bfloat16),
            pltpu.VMEM((4, 256, 128), jnp.bfloat16),
            pltpu.SemaphoreType.DMA((4,)),
            pltpu.SemaphoreType.DMA((4,)),
            pltpu.SemaphoreType.DMA((15,)),
            pltpu.SemaphoreType.DMA((15,)),
            pltpu.SemaphoreType.DMA,
            pltpu.SemaphoreType.DMA,
            pltpu.SemaphoreType.DMA((2,)),
        ],
        compiler_params=pltpu.CompilerParams(
            collective_id=1, has_side_effects=True, vmem_limit_bytes=60 * 1024 * 1024
        ),
        name="close",
    )(heads, o_full, tokens_t, ids, router, bias, gain)


def finish_kernel(got, out, gates):
    spot = pl.program_id(0)
    lanes_here = got.shape[2]
    halves = []
    for part in range(2):
        rows = got[part * 64 : part * 64 + 64].reshape(512, lanes_here)
        source = lax.broadcasted_iota(jnp.int32, (512, 512), 0)
        target = lax.broadcasted_iota(jnp.int32, (512, 512), 1)
        pick = (source == (target & 63) * 8 + (target >> 6)).astype(jnp.bfloat16)
        halves.append(
            lax.dot_general(rows, pick, (((0,), (0,)), ((), ())), preferred_element_type=jnp.float32)
        )
    whole = []
    for c in range(8):
        cut = slice(c * 64, c * 64 + 64)
        whole.append(jnp.concatenate([halves[0][:, cut], halves[1][:, cut]], axis=1))
        out[c] = whole[c].astype(jnp.bfloat16)

    @pl.when(spot == WIDTH // FINISH_LANES)
    def _():
        mine = lax.axis_index("expert").astype(jnp.float32)
        first = WIDTH % FINISH_LANES
        found = []
        for c in range(8):
            data = whole[c][first : first + 8]
            asked = jnp.where(data[4:8] == mine, data[:4], 0.0)
            found.append(jnp.sum(asked, axis=0, keepdims=True))
        gates[...] = jnp.concatenate(found, axis=0).astype(jnp.bfloat16)


def finish(got):
    return pl.pallas_call(
        finish_kernel,
        grid=(-(-WIDE // FINISH_LANES),),
        out_shape=[
            jax.ShapeDtypeStruct((8, WIDTH, 128), jnp.bfloat16),
            jax.ShapeDtypeStruct((8, 128), jnp.bfloat16),
        ],
        in_specs=[pl.BlockSpec((128, 8, FINISH_LANES), lambda i: (0, 0, i))],
        out_specs=[
            pl.BlockSpec((8, FINISH_LANES, 128), lambda i: (0, i, 0)),
            pl.BlockSpec((8, 128), lambda i: (0, 0)),
        ],
        name="finish",
    )(got)


def on_device(
    tokens,
    segment_ids,
    expert_ids,
    attn_gain,
    sinks,
    qkv_master,
    qkv_mom,
    qkv_var,
    qkv_grad,
    o_master,
    o_mom,
    o_var,
    o_grad,
    router_weight,
    router_bias,
    mlp_gain,
):
    tok_rows = tokens.shape[0]
    qkv_local = adam_weights(qkv_master, qkv_mom, qkv_var, qkv_grad)
    o_local = adam_weights(o_master, o_mom, o_var, o_grad)
    positions = jnp.arange(tok_rows).astype(jnp.float32)
    spread = jnp.arange(HEAD_DIM // 2).astype(jnp.float32) * 2.0 / HEAD_DIM
    angles = (rope_base**-spread)[:, None] * positions[None, :]
    o_full, heads = open_up(
        qkv_local[:8],
        qkv_local[8:],
        o_local,
        tokens.T,
        attn_gain[None, :],
        segment_ids[None, :],
        sinks[None, :],
        jnp.cos(angles),
        jnp.sin(angles),
    )
    got = close(
        heads,
        o_full.reshape(-1, WIDTH),
        tokens.T,
        expert_ids.T,
        router_weight,
        router_bias[None, :],
        mlp_gain[None, :],
    )
    dispatched, gates = finish(got)
    dispatched = jnp.transpose(dispatched, (2, 0, 1))[None, :, None]
    gates = jnp.transpose(gates)[None, :, None]
    return (dispatched, gates)


def solution(mesh):
    return jax.shard_map(
        on_device,
        mesh=mesh,
        in_specs=(
            P("expert", None),
            P("expert"),
            P("expert", None),
            P(),
            P("dp"),
            P(("dp", "expert"), None),
            P(("dp", "expert"), None),
            P(("dp", "expert"), None),
            P(("dp", "expert"), None),
            P(("dp", "expert"), None),
            P(("dp", "expert"), None),
            P(("dp", "expert"), None),
            P(("dp", "expert"), None),
            P(),
            P(),
            P(),
        ),
        out_specs=(P("expert", None, "dp", None, None), P("expert", None, "dp", None)),
        check_vma=False,
    )
```

```python
import jax
import jax.numpy as jnp
import numpy as np
from jax import lax
from jax.experimental import pallas as pl
from jax.experimental.pallas import tpu as pltpu
from jax.sharding import PartitionSpec as P

HEAD_DIM = 64
WINDOW = 128
WIDTH = 2880
WIDE = 2944
HALF = 1408
META = 2816
MESH = pl.DeviceIdType.MESH
FINISH_LANES = 768

beta_one = 0.9
beta_two = 0.999
adam_step = 100
learn_rate = 0.02
adam_eps = 1e-08
norm_eps = 1e-05
rope_base = 150000.0


def adam_weights(master, moment, second_mom, gradient):
    moment_new = beta_one * moment + (1.0 - beta_one) * gradient
    second_new = beta_two * second_mom + (1.0 - beta_two) * gradient * gradient
    fix_one = 1.0 - beta_one**adam_step
    fix_two = 1.0 - beta_two**adam_step
    update = moment_new / fix_one / (jnp.sqrt(second_new / fix_two) + adam_eps)
    return master - learn_rate * update


def place():
    e = lax.axis_index("expert")
    core = lax.rem(e, 2)
    x = lax.rem(lax.div(e, 2), 4)
    z = lax.rem(lax.div(e, 8), 4)
    y = lax.div(e, 32)
    return e, y, z, x, core


def expert_at(y, z, x, core):
    return y * 32 + z * 8 + x * 2 + core


def step(position, by):
    return lax.rem(position + by, 4)


def greet(peers):
    barrier = pltpu.get_barrier_semaphore()
    for peer in peers:
        pl.semaphore_signal(barrier, inc=1, device_id={"expert": peer}, device_id_type=MESH)
    pl.semaphore_wait(barrier, len(peers))


def remote(src, dst, send_sem, recv_sem, peer):
    return pltpu.make_async_remote_copy(
        src_ref=src,
        dst_ref=dst,
        send_sem=send_sem,
        recv_sem=recv_sem,
        device_id={"expert": peer},
        device_id_type=MESH,
    )


def gathered_experts():
    core, last, middle, z = np.meshgrid(
        np.arange(2), np.arange(4), np.arange(4), np.arange(4), indexing="ij"
    )
    y = np.where(core == 0, middle, last)
    x = np.where(core == 0, last, middle)
    return (((y * 4 + z) * 4 + x) * 2 + core).reshape(-1)


def open_kernel(
    qkv_state,
    qkv_mom,
    qkv_var,
    qkv_grad,
    o_state,
    o_mom,
    o_var,
    o_grad,
    tokens,
    gain,
    segments,
    sinks,
    cosine,
    sine,
    go,
    heads,
    a,
    b,
    o,
    tokens_t,
    ga,
    gb,
    normed,
    from_eight,
    from_two,
    two_rows,
    projected,
    attended,
    send,
    recv,
    local,
):
    _, y, z, x, core = place()
    middle = y * (1 - core) + x * core
    last = x * (1 - core) + y * core

    def peer(last_at, middle_at, z_at):
        return expert_at(
            middle_at * (1 - core) + last_at * core,
            z_at,
            last_at * (1 - core) + middle_at * core,
            core,
        )

    partner = expert_at(y, z, x, 1 - core)
    ring = [
        (peer(last, middle, step(z, 1)), peer(last, middle, step(z, 3))),
        (peer(last, step(middle, 1), z), peer(last, step(middle, 3), z)),
        (peer(step(last, 1), middle, z), peer(step(last, 3), middle, z)),
    ]
    for start in range(0, WIDTH, 640):
        lanes = slice(start, min(start + 640, WIDTH))
        updated = adam_weights(
            qkv_state[:, lanes], qkv_mom[:, lanes], qkv_var[:, lanes], qkv_grad[:, lanes]
        )
        a[:, lanes] = updated[:8].astype(jnp.bfloat16)
        b[:, lanes] = updated[8:].astype(jnp.bfloat16)
        o[:, lanes] = adam_weights(
            o_state[:, lanes], o_mom[:, lanes], o_var[:, lanes], o_grad[:, lanes]
        ).astype(jnp.bfloat16)
    greet([p for pair in ring for p in pair] + [partner])
    streams = ((a, ga), (b, gb), (o, go))
    copies = {}
    fetch = pltpu.make_async_copy(tokens, tokens_t, local.at[3])
    fetch.start()

    def move(s, tag, src, dst, to):
        k = sum(1 for key in copies if key[0] == s)
        copy = remote(src, dst, send.at[s, k], recv.at[s, k], to)
        copy.start()
        copies[s, tag] = copy

    def arrived(s, tag):
        copies[s, tag].wait_recv()

    fine = ((0, 0, 4), (3, 0, 4), (1, 0, 4), (2, 0, 2), (2, 2, 2))
    coarse = (None,)
    pieces = (fine, coarse, fine)

    def part(s, last_by, k):
        full = streams[s][1]
        piece = pieces[s][k]
        if piece is None:
            return full.at[core, step(last, last_by)]
        return full.at[core, step(last, last_by), step(middle, piece[0]), pl.ds(piece[1], piece[2])]

    def along_last(s, k):
        block = part(s, 0, k)
        move(s, ("last", k, 0), block, block, ring[2][0])
        move(s, ("last", k, 1), block, block, ring[2][1])
        move(s, ("pair", 0, k), block, block, partner)

    def from_last(s, k):
        count = len(pieces[s])
        low, high = part(s, 3, k), part(s, 1, k)
        arrived(s, ("last", k, 0))
        if k < 2 and count > 1:
            move(s, ("far", k), low, low, ring[2][0])
        move(s, ("pair", 3, k), low, low, partner)
        arrived(s, ("last", k, 1))
        if k >= 2 or count == 1:
            move(s, ("far", k), high, high, ring[2][1])
        move(s, ("pair", 1, k), high, high, partner)

    own = []
    for s, (shard, full) in enumerate(streams):
        mine = full.at[core, last, middle, z]
        move(s, "z up", shard, mine, ring[0][0])
        move(s, "z down", shard, mine, ring[0][1])
        copy = pltpu.make_async_copy(shard, mine, local.at[s])
        copy.start()
        own.append(copy)
    for s, (_, full) in enumerate(streams):
        if s < 2:
            arrived(s, "z up")
            block = full.at[core, last, middle, step(z, 3)]
            move(s, "z far", block, block, ring[0][0])
        else:
            arrived(s, "z down")
            block = full.at[core, last, middle, step(z, 1)]
            move(s, "z far", block, block, ring[0][1])
    for s, (_, full) in enumerate(streams):
        arrived(s, "z down" if s < 2 else "z up")
        arrived(s, "z far")
        own[s].wait()
        block = full.at[core, last, middle]
        move(s, "middle up", block, block, ring[1][0])
        move(s, "middle down", block, block, ring[1][1])
        if s == 0:
            along_last(s, 0)
    for s, (_, full) in enumerate(streams):
        arrived(s, "middle up")
        block = full.at[core, last, step(middle, 3), pl.ds(0, 2)]
        move(s, "middle far 0", block, block, ring[1][0])
        if s == 0:
            along_last(s, 1)
        arrived(s, "middle down")
        block = full.at[core, last, step(middle, 1), pl.ds(2, 2)]
        move(s, "middle far 1", block, block, ring[1][1])
        if s == 0:
            along_last(s, 2)
    for s in range(3):
        arrived(s, "middle far 0")
        if s == 0:
            along_last(s, 3)
        arrived(s, "middle far 1")
        if s < 2:
            along_last(s, 4 if s == 0 else 0)
    fetch.wait()
    square = jnp.zeros((1, 256), jnp.float32)
    for start in range(0, WIDTH, 192):
        chunk = tokens_t[start : start + 192].astype(jnp.float32)
        square = square + jnp.sum(chunk * chunk, axis=0, keepdims=True)
    scale = lax.rsqrt(square * (1.0 / WIDTH) + norm_eps)
    for start in range(0, WIDTH, 128):
        size = min(128, WIDTH - start)
        column = jnp.broadcast_to(gain[0:1, start : start + size], (128, size)).T
        for half in range(2):
            lanes = slice(half * 128, half * 128 + 128)
            chunk = tokens_t[start : start + size, lanes].astype(jnp.float32)
            normed[start : start + size, lanes] = (chunk * scale[:, lanes] * column).astype(
                jnp.bfloat16
            )
    for k in range(5):
        from_last(0, k)
        if k == 0:
            from_last(1, 0)
        if k >= 2:
            along_last(2, k - 2)
    along_last(2, 3)
    along_last(2, 4)

    def from_far(s, k):
        block = part(s, 2, k)
        arrived(s, ("far", k))
        move(s, ("pair", 2, k), block, block, partner)

    for k in range(5):
        from_far(0, k)
    from_far(1, 0)

    def output_step(n):
        if n < 5:
            from_last(2, n)
        elif n < 10:
            from_far(2, n - 5)

    for (s, tag), copy in copies.items():
        if s < 2 and tag[0] == "pair":
            copy.wait_recv()
    output_step(0)
    order = gathered_experts()
    for n in range(128):
        two = gb[n // 64, n // 16 % 4, n // 4 % 4, n % 4]
        two_rows[n * 2 : n * 2 + 2] = two.astype(jnp.float32)
    output_step(1)
    from_two[...] = jnp.dot(
        two_rows[...].astype(jnp.bfloat16), normed[...], preferred_element_type=jnp.float32
    )
    for n in range(4):
        rows = ga[n // 2, n % 2 * 2 : n % 2 * 2 + 2].reshape(256, WIDTH)
        from_eight[n * 256 : n * 256 + 256] = jnp.dot(
            rows, normed[...], preferred_element_type=jnp.float32
        )
        if n % 2 == 1:
            output_step(2 + n // 2)
    for g in range(128):
        row = int(order[g]) * 10
        projected[row : row + 8] = from_eight[g * 8 : g * 8 + 8]
        projected[row + 8 : row + 10] = from_two[g * 2 : g * 2 + 2]
    output_step(4)

    def turn(row):
        first, second = projected[row : row + 32], projected[row + 32 : row + 64]
        return jnp.concatenate(
            [
                first * cosine[...] - second * sine[...],
                second * cosine[...] + first * sine[...],
            ],
            axis=0,
        )

    owner = segments[...].astype(jnp.float32)
    other = jnp.concatenate(
        [jnp.broadcast_to(owner[:, h * 128 : h * 128 + 128], (128, 128)).T for h in range(2)], axis=0
    )
    other = jnp.concatenate([other, other], axis=1)
    behind = lax.broadcasted_iota(jnp.int32, (256, 256), 1) - lax.broadcasted_iota(
        jnp.int32, (256, 256), 0
    )
    allowed = (other == owner) & (behind >= 0) & (behind < WINDOW)
    allowed = allowed.astype(jnp.float32)
    for kv in range(2):
        keys = turn(1024 + kv * 64).T.astype(jnp.bfloat16)
        values = projected[1152 + kv * 64 : 1216 + kv * 64].astype(jnp.bfloat16)
        for h in range(kv * 8, kv * 8 + 8):
            if h % 4 == 0:
                output_step(h // 4 + 5)
            queries = turn(h * 64).astype(jnp.bfloat16)
            scores = jnp.dot(keys, queries, preferred_element_type=jnp.float32)
            shares = jnp.where(allowed > 0.0, jnp.exp(scores * HEAD_DIM**-0.5), 0.0)
            running = jnp.exp(sinks[:, h : h + 1]) + jnp.sum(shares, axis=0, keepdims=True)
            probs = (shares * (1.0 / running)).astype(jnp.bfloat16)
            attended[h * 64 : h * 64 + 64] = jnp.dot(
                values, probs, preferred_element_type=jnp.float32
            )
    output_step(9)
    for j in range(8):
        cut = jnp.concatenate(
            [
                attended[int(order[g]) * 8 : int(order[g]) * 8 + 8]
                for g in range(j * 16, j * 16 + 16)
            ],
            axis=0,
        )
        for half in range(2):
            heads[half * 128 : half * 128 + 128, j * 128 : j * 128 + 128] = (
                cut[:, half * 128 : half * 128 + 128].T.astype(jnp.bfloat16)
            )
    for (s, tag), copy in copies.items():
        if s == 2 and tag[0] == "pair":
            copy.wait_recv()
    for copy in copies.values():
        copy.wait_send()


def open_up(*operands):
    return pl.pallas_call(
        open_kernel,
        out_shape=[
            jax.ShapeDtypeStruct((2, 4, 4, 4, 8, WIDTH), jnp.bfloat16),
            jax.ShapeDtypeStruct((256, 1024), jnp.bfloat16),
        ],
        in_specs=[pl.BlockSpec(memory_space=pltpu.VMEM)] * 8
        + [pl.BlockSpec(memory_space=pltpu.HBM)]
        + [pl.BlockSpec(memory_space=pltpu.VMEM)] * 5,
        out_specs=[
            pl.BlockSpec(memory_space=pl.ANY),
            pl.BlockSpec(memory_space=pltpu.VMEM),
        ],
        scratch_shapes=[
            pltpu.VMEM((8, WIDTH), jnp.bfloat16),
            pltpu.VMEM((2, WIDTH), jnp.bfloat16),
            pltpu.VMEM((8, WIDTH), jnp.bfloat16),
            pltpu.VMEM((WIDTH, 256), jnp.bfloat16),
            pltpu.VMEM((2, 4, 4, 4, 8, WIDTH), jnp.bfloat16),
            pltpu.VMEM((2, 4, 4, 4, 2, WIDTH), jnp.bfloat16),
            pltpu.VMEM((WIDTH, 256), jnp.bfloat16),
            pltpu.VMEM((1024, 256), jnp.float32),
            pltpu.VMEM((256, 256), jnp.float32),
            pltpu.VMEM((256, WIDTH), jnp.float32),
            pltpu.VMEM((1280, 256), jnp.float32),
            pltpu.VMEM((1024, 256), jnp.float32),
            pltpu.SemaphoreType.DMA((3, 42)),
            pltpu.SemaphoreType.DMA((3, 42)),
            pltpu.SemaphoreType.DMA((4,)),
        ],
        compiler_params=pltpu.CompilerParams(
            collective_id=0, has_side_effects=True, vmem_limit_bytes=60 * 1024 * 1024
        ),
        name="open",
    )(*operands)


PARTS = ((0, 768), (768, 768), (1536, 768), (2304, 640))


def close_kernel(
    heads,
    o_there,
    tokens,
    ids,
    router,
    bias,
    gain,
    got,
    o_full,
    tokens_t,
    rows,
    total,
    partial,
    landed,
    ring_rows,
    payload,
    picks,
    psend,
    precv,
    zsend,
    zrecv,
    send_sem,
    recv_sem,
    local,
):
    fetches = [
        pltpu.make_async_copy(src, dst, local.at[k])
        for k, (src, dst) in enumerate(((o_there, o_full), (tokens, tokens_t)))
    ]
    for copy in fetches:
        copy.start()
    e, y, z, x, core = place()
    group = lax.axis_index("dp")
    here = y * 8 + x * 2 + core
    above, below = expert_at(y, step(z, 1), x, core), expert_at(y, step(z, 3), x, core)

    def plane_expert(index):
        return lax.div(index, 8) * 32 + z * 8 + lax.rem(index, 8)

    barrier = pltpu.get_barrier_semaphore()
    other = {"dp": 1 - group, "expert": e}
    pl.semaphore_signal(barrier, inc=1, device_id=other, device_id_type=MESH)
    for peer in (above, below):
        pl.semaphore_signal(barrier, inc=1, device_id={"expert": peer}, device_id_type=MESH)

    def signal_one(i, carry):
        peer = plane_expert(lax.rem(here + i, 32))
        pl.semaphore_signal(barrier, inc=1, device_id={"expert": peer}, device_id_type=MESH)
        return carry

    lax.fori_loop(1, 32, signal_one, 0)
    pl.semaphore_wait(barrier, 34)

    block, tail_tile = 128, pl.ds(META, 128)
    mine = pl.ds(pl.multiple_of(group * block, block), block)
    theirs = pl.ds(pl.multiple_of((1 - group) * block, block), block)
    partial[:, tail_tile] = jnp.zeros((block, 128), jnp.bfloat16)
    total[:, tail_tile] = jnp.zeros((block, 128), jnp.float32)
    exchanges = []
    fetches[0].wait()
    for n, (start, lanes_here) in enumerate(PARTS):
        inside = pl.ds(start, min(lanes_here, WIDTH - start))
        update = jnp.dot(heads[theirs, :], o_full[:, inside], preferred_element_type=jnp.float32)
        partial[:, inside] = update.astype(jnp.bfloat16)
        lanes = pl.ds(start, lanes_here)
        copy = pltpu.make_async_remote_copy(
            src_ref=partial.at[:, lanes],
            dst_ref=landed.at[:, lanes],
            send_sem=psend.at[n],
            recv_sem=precv.at[n],
            device_id=other,
            device_id_type=MESH,
        )
        copy.start()
        exchanges.append(copy)
    for start, lanes_here in PARTS:
        inside = pl.ds(start, min(lanes_here, WIDTH - start))
        total[:, inside] = jnp.dot(
            heads[mine, :], o_full[:, inside], preferred_element_type=jnp.float32
        )
    fetches[1].wait()
    for start in range(0, WIDTH, 128):
        inside = pl.ds(start, min(128, WIDTH - start))
        total[:, inside] = total[:, inside] + tokens_t[inside, mine].astype(jnp.float32).T

    number = lax.broadcasted_iota(jnp.int32, (block, 128), 1)
    row_number = lax.broadcasted_iota(jnp.int32, (block, 128), 0)
    chosen = [(ids[k : k + 1, mine] == row_number).astype(jnp.float32).T for k in range(4)]
    named = (chosen[0] + chosen[1] + chosen[2] + chosen[3]).astype(jnp.bfloat16)
    earlier = jnp.dot(
        (number < row_number).astype(jnp.bfloat16), named, preferred_element_type=jnp.float32
    )
    expert = number.astype(jnp.float32)
    first_slot = ((number >> 5) * 64 + (number & 7) * 8).astype(jnp.float32) + earlier
    plane_of = ((number >> 3) & 3).astype(jnp.float32)
    extra = jnp.zeros((block, 128), jnp.float32)
    for k in range(4):
        for at, what in ((68, expert), (72, first_slot), (76, plane_of)):
            value = jnp.sum(chosen[k] * what, axis=1, keepdims=True)
            extra = jnp.where(number == at + k, value, extra)

    def choose(block, data):
        code = lax.broadcasted_iota(jnp.int32, (128, 256), 1).astype(jnp.float32)
        plane = z.astype(jnp.float32)
        hit = jnp.zeros((128, 256), jnp.float32)
        for k in range(4):
            same = (data[:, 72 + k : 73 + k] == code) & (data[:, 76 + k : 77 + k] == plane)
            hit = hit + jnp.where(same, 1.0, 0.0)
        picks[block] = hit.T.astype(jnp.bfloat16)

    choose(0, extra)
    square = jnp.zeros((block, 1), jnp.float32)
    for copy, (start, lanes_here) in zip(exchanges, PARTS):
        copy.wait_recv()
        lanes = pl.ds(start, lanes_here)
        residual = total[:, lanes] + landed[:, lanes].astype(jnp.float32)
        total[:, lanes] = residual
        square = square + jnp.sum(residual * residual, axis=1, keepdims=True)
    scale = lax.rsqrt(square * (1.0 / WIDTH) + norm_eps)
    for start, lanes_here in PARTS:
        inside = pl.ds(start, min(lanes_here, WIDTH - start))
        rows[:, inside] = (total[:, inside] * scale * gain[:, inside]).astype(jnp.bfloat16)

    def route():
        logits = bias[...] + jnp.zeros((block, 128), jnp.float32)
        for start, lanes_here in PARTS:
            inside = pl.ds(start, min(lanes_here, WIDTH - start))
            logits = logits + jnp.dot(
                rows[:, inside], router[inside, :], preferred_element_type=jnp.float32
            )
        raised = [
            jnp.exp(jnp.sum(jnp.where(chosen[k] > 0.0, logits, 0.0), axis=1, keepdims=True))
            for k in range(4)
        ]
        norm = raised[0] + raised[1] + raised[2] + raised[3]
        whole = extra
        for k in range(4):
            whole = jnp.where(number == 64 + k, raised[k] / norm, whole)
        rows[:, tail_tile] = jnp.where(
            number < WIDTH - META, rows[:, tail_tile].astype(jnp.float32), whole
        ).astype(jnp.bfloat16)

    meta = pl.ds(META, 128)
    chunks = ((0, 768), (768, 768), (1536, 768), (2304, 512))
    from_low, from_high, from_far = ring_rows.at[0], ring_rows.at[1], ring_rows.at[2]

    def pass_on(k, src, slot, lanes, peer):
        copy = remote(
            src.at[:, lanes], ring_rows.at[slot, :, lanes], zsend.at[k], zrecv.at[k], peer
        )
        copy.start()
        return copy

    def leg(n):
        if n < 4:
            up = pass_on(2 * n, rows, 0, pl.ds(*chunks[n]), above)
            down = pass_on(2 * n + 1, rows, 1, pl.ds(*chunks[3 - n]), below)
        else:
            up = pass_on(2 * n, from_low, 2, pl.ds(*chunks[n - 4]), above)
            down = pass_on(2 * n + 1, from_high, 2, pl.ds(*chunks[7 - n]), below)
        return up, down

    legs = [leg(0)]

    def deliver(block, source, z_at, chunk):
        start, lanes_here = chunks[chunk]
        lanes_here = lanes_here if chunk < 3 else WIDE - start
        for at in range(0, lanes_here, 384):
            lanes = pl.ds(start + at, min(384, lanes_here - at))
            slots = jnp.dot(picks[block], source[:, lanes], preferred_element_type=jnp.float32)
            payload[block, :, :, lanes] = slots.reshape(32, 8, -1).astype(jnp.bfloat16)
        lanes = pl.ds(start, lanes_here)
        row = expert_at(y, z_at, x, core)
        pltpu.make_async_copy(
            payload.at[block, here, :, lanes], got.at[row, :, lanes], recv_sem
        ).start()

        def one(i, carry):
            index = lax.rem(here + i, 32)
            remote(
                payload.at[block, index, :, lanes],
                got.at[row, :, lanes],
                send_sem,
                recv_sem,
                plane_expert(index),
            ).start()
            return carry

        lax.fori_loop(1, 32, one, 0)

    deliver(0, rows, z, 0)
    route()
    low_meta = pass_on(12, rows, 0, meta, above)
    high_meta = pass_on(13, rows, 1, meta, below)
    for chunk in range(1, 4):
        deliver(0, rows, z, chunk)
    low_meta.wait_recv()
    far_meta = pass_on(14, from_low, 2, meta, above)
    high_meta.wait_recv()
    choose(1, from_low[:, META:WIDE].astype(jnp.float32))
    choose(2, from_high[:, META:WIDE].astype(jnp.float32))
    for n in range(6):
        up, down = legs[n]
        if n < 5:
            up.wait_send()
            down.wait_send()
            legs.append(leg(n + 1))
        if n == 3:
            far_meta.wait_recv()
            choose(3, from_far[:, META:WIDE].astype(jnp.float32))
        up.wait_recv()
        deliver(*((1, from_low, step(z, 3), n) if n < 4 else (3, from_far, step(z, 2), n - 4)))
        down.wait_recv()
        deliver(*((2, from_high, step(z, 1), 3 - n) if n < 4 else (3, from_far, step(z, 2), 7 - n)))
    pltpu.make_async_copy(got, got, recv_sem).wait()
    part = payload.at[:, pl.ds(0, 31)]
    pltpu.make_async_copy(part, part, send_sem).wait()
    for copy in (low_meta, high_meta, far_meta, *legs[5], *exchanges):
        copy.wait_send()


def close(heads, o_full, tokens_t, ids, router, bias, gain):
    return pl.pallas_call(
        close_kernel,
        out_shape=jax.ShapeDtypeStruct((128, 8, WIDE), jnp.bfloat16),
        in_specs=[pl.BlockSpec(memory_space=pltpu.VMEM)]
        + [pl.BlockSpec(memory_space=pltpu.HBM)] * 2
        + [pl.BlockSpec(memory_space=pltpu.VMEM)] * 4,
        out_specs=pl.BlockSpec(memory_space=pl.ANY),
        scratch_shapes=[
            pltpu.VMEM((1024, WIDTH), jnp.bfloat16),
            pltpu.VMEM((WIDTH, 256), jnp.bfloat16),
            pltpu.VMEM((128, WIDE), jnp.bfloat16),
            pltpu.VMEM((128, WIDE), jnp.float32),
            pltpu.VMEM((128, WIDE), jnp.bfloat16),
            pltpu.VMEM((128, WIDE), jnp.bfloat16),
            pltpu.VMEM((3, 128, WIDE), jnp.bfloat16),
            pltpu.VMEM((4, 32, 8, WIDE), jnp.bfloat16),
            pltpu.VMEM((4, 256, 128), jnp.bfloat16),
            pltpu.SemaphoreType.DMA((4,)),
            pltpu.SemaphoreType.DMA((4,)),
            pltpu.SemaphoreType.DMA((15,)),
            pltpu.SemaphoreType.DMA((15,)),
            pltpu.SemaphoreType.DMA,
            pltpu.SemaphoreType.DMA,
            pltpu.SemaphoreType.DMA((2,)),
        ],
        compiler_params=pltpu.CompilerParams(
            collective_id=1, has_side_effects=True, vmem_limit_bytes=60 * 1024 * 1024
        ),
        name="close",
    )(heads, o_full, tokens_t, ids, router, bias, gain)


def finish_kernel(got, out, gates):
    spot = pl.program_id(0)
    lanes_here = got.shape[2]
    halves = []
    source = lax.broadcasted_iota(jnp.int32, (512, 512), 0)
    target = lax.broadcasted_iota(jnp.int32, (512, 512), 1)
    pick = (source == (target & 63) * 8 + (target >> 6)).astype(jnp.bfloat16)
    for part in range(2):
        rows = got[part * 64 : part * 64 + 64].reshape(512, lanes_here)
        halves.append(
            lax.dot_general(rows, pick, (((0,), (0,)), ((), ())), preferred_element_type=jnp.float32)
        )
    whole = []
    for c in range(8):
        cut = slice(c * 64, c * 64 + 64)
        whole.append(jnp.concatenate([halves[0][:, cut], halves[1][:, cut]], axis=1))
        out[c] = whole[c].astype(jnp.bfloat16)

    @pl.when(spot == WIDTH // FINISH_LANES)
    def _():
        mine = lax.axis_index("expert").astype(jnp.float32)
        first = WIDTH % FINISH_LANES
        found = []
        for c in range(8):
            data = whole[c][first : first + 8]
            asked = jnp.where(data[4:8] == mine, data[:4], 0.0)
            found.append(jnp.sum(asked, axis=0, keepdims=True))
        gates[...] = jnp.concatenate(found, axis=0).astype(jnp.bfloat16)


def finish(got):
    return pl.pallas_call(
        finish_kernel,
        grid=(-(-WIDE // FINISH_LANES),),
        out_shape=[
            jax.ShapeDtypeStruct((8, WIDTH, 128), jnp.bfloat16),
            jax.ShapeDtypeStruct((8, 128), jnp.bfloat16),
        ],
        in_specs=[pl.BlockSpec((128, 8, FINISH_LANES), lambda i: (0, 0, i))],
        out_specs=[
            pl.BlockSpec((8, FINISH_LANES, 128), lambda i: (0, i, 0)),
            pl.BlockSpec((8, 128), lambda i: (0, 0)),
        ],
        name="finish",
    )(got)


def on_device(
    tokens,
    segment_ids,
    expert_ids,
    attn_gain,
    sinks,
    qkv_master,
    qkv_mom,
    qkv_var,
    qkv_grad,
    o_master,
    o_mom,
    o_var,
    o_grad,
    router_weight,
    router_bias,
    mlp_gain,
):
    tok_rows = tokens.shape[0]
    positions = jnp.arange(tok_rows).astype(jnp.float32)
    spread = jnp.arange(HEAD_DIM // 2).astype(jnp.float32) * 2.0 / HEAD_DIM
    angles = (rope_base**-spread)[:, None] * positions[None, :]
    o_full, heads = open_up(
        qkv_master,
        qkv_mom,
        qkv_var,
        qkv_grad,
        o_master,
        o_mom,
        o_var,
        o_grad,
        tokens.T,
        attn_gain[None, :],
        segment_ids[None, :],
        sinks[None, :],
        jnp.cos(angles),
        jnp.sin(angles),
    )
    got = close(
        heads,
        o_full.reshape(-1, WIDTH),
        tokens.T,
        expert_ids.T,
        router_weight,
        router_bias[None, :],
        mlp_gain[None, :],
    )
    dispatched, gates = finish(got)
    dispatched = jnp.transpose(dispatched, (2, 0, 1))[None, :, None]
    gates = jnp.transpose(gates)[None, :, None]
    return (dispatched, gates)


def solution(mesh):
    return jax.shard_map(
        on_device,
        mesh=mesh,
        in_specs=(
            P("expert", None),
            P("expert"),
            P("expert", None),
            P(),
            P("dp"),
            P(("dp", "expert"), None),
            P(("dp", "expert"), None),
            P(("dp", "expert"), None),
            P(("dp", "expert"), None),
            P(("dp", "expert"), None),
            P(("dp", "expert"), None),
            P(("dp", "expert"), None),
            P(("dp", "expert"), None),
            P(),
            P(),
            P(),
        ),
        out_specs=(P("expert", None, "dp", None, None), P("expert", None, "dp", None)),
        check_vma=False,
    )
```
